32 devices in a mesh: dp: 2 (over core), tensor: 16 (over z, y, x).
Axes of the slice: x: 2, y: 2, z: 4, core: 2. Of those that a mesh axis runs over, the one named last changes fastest.
Arguments:
- gradient: float32 [2, 8192, 512], P('dp', 'tensor'), may hold values from -80 to 80
Outputs:
- update: bfloat16 [2, 8192, 512], P(None, 'tensor')
The draws below stay inside these ranges and needn't reach their ends.
All inputs are finite; a program needn't handle non-finite values.
Results may differ from the reference program's by a relative error of at most 0.001.
Values may be sent and summed in bfloat16 or wider, within the bound.
No kernel may reach another device: no remote copies, remote signals or barrier semaphores. Data moves between devices by JAX's collectives and lax.ppermute only.
A program may use at most 64 MiB of HBM per device.

```python
import math
import jax
import jax.numpy as jnp
from jax import lax

FEATURES = 8192
OUTPUTS = 512
ITERS = 3
MATS = 2


def draw_gradient(key, part):
    keys = jax.random.split(jax.random.fold_in(key, 17), 5)
    ramp = 1.0 + 2.0 * jnp.arange(FEATURES, dtype=jnp.float32) / (FEATURES - 1)
    feature_scale = jnp.exp(jax.random.uniform(keys[0], (MATS, FEATURES, 1), jnp.float32, 0.0, math.log(10.0))) * ramp[None, :, None]
    output_scale = jnp.exp(jax.random.uniform(keys[1], (MATS, 1, OUTPUTS), jnp.float32, 0.0, math.log(10.0)))
    common = jax.random.truncated_normal(keys[2], -6.0, 6.0, (MATS, 1, OUTPUTS), jnp.float32)
    bulk = jax.random.truncated_normal(keys[4], -6.0, 6.0, (MATS, FEATURES, OUTPUTS), jnp.float32)
    return 0.01 * feature_scale * output_scale * (bulk + 0.35 * common)


def setup_inputs(seed: int = 0) -> dict:
    key_of = jax.random.split(jax.random.key(seed), 2)
    gradient = draw_gradient(jax.random.fold_in(key_of[1], 71), 0)
    return dict(gradient=gradient)


linear_term = 3.4445
cubic_term = -4.775
quintic_term = 2.0315
norm_floor = 1e-07
update_gain = 0.2

def multiply(first_factor, second_factor):
    return jnp.einsum('mrs,mst->mrt', first_factor, second_factor, precision=lax.Precision.HIGHEST)

def reference(gradient):
    squared_norm = lax.optimization_barrier(jnp.sum(gradient * gradient, axis=(1, 2)))
    divisor = jnp.sqrt(squared_norm) + norm_floor
    raw_gram = jnp.einsum('mfr,mfs->mrs', gradient, gradient, precision=lax.Precision.HIGHEST)
    gram_matrix = raw_gram / (divisor * divisor)[:, None, None]
    identity = jnp.eye(OUTPUTS, dtype=jnp.float32)[None]
    running = identity
    for turn_index in range(ITERS):
        squared = multiply(gram_matrix, gram_matrix)
        polynomial = linear_term * identity + cubic_term * gram_matrix + quintic_term * squared
        if turn_index == 0:
            running = polynomial
        else:
            running = multiply(running, polynomial)
        if turn_index + 1 < ITERS:
            gram_matrix = multiply(multiply(polynomial, gram_matrix), polynomial)
    polished = jnp.einsum('mfr,mrs->mfs', gradient, running, precision=lax.Precision.HIGHEST)
    factor = update_gain * math.sqrt(max(FEATURES, OUTPUTS)) / divisor
    return (factor[:, None, None] * polished).astype(jnp.bfloat16)
```

```python
import math

import jax
import jax.numpy as jnp
from jax import lax
from jax.sharding import PartitionSpec as P

FEATURES = 8192
OUTPUTS = 512
ITERS = 3


linear_term = 3.4445
cubic_term = -4.775
quintic_term = 2.0315
norm_floor = 1e-07
update_gain = 0.2


def multiply(first_factor, second_factor):
    return jnp.einsum("mrs,mst->mrt", first_factor, second_factor, precision=lax.Precision.HIGHEST)


def local_gram(gradient):
    return jnp.einsum("mfr,mfs->mrs", gradient, gradient, precision=lax.Precision.HIGHEST)


def reduce_gram(partial_gram):
    return lax.psum(partial_gram, "tensor")


def replicated_total(gram_matrix):
    order = gram_matrix.shape[2]
    identity = jnp.eye(order, dtype=jnp.float32)[None]
    running = identity
    for turn_index in range(ITERS):
        squared = multiply(gram_matrix, gram_matrix)
        polynomial = linear_term * identity + cubic_term * gram_matrix + quintic_term * squared
        if turn_index == 0:
            running = polynomial
        else:
            running = multiply(running, polynomial)
        if turn_index + 1 < ITERS:
            gram_matrix = multiply(multiply(polynomial, gram_matrix), polynomial)
    return running


def on_device(gradient):
    summed = reduce_gram(local_gram(gradient))
    squared_norm = jnp.trace(summed, axis1=1, axis2=2)
    divisor = jnp.sqrt(squared_norm) + norm_floor
    gram_matrix = summed / (divisor * divisor)[:, None, None]
    polished = jnp.einsum(
        "mfr,mrs->mfs", gradient, replicated_total(gram_matrix), precision=lax.Precision.HIGHEST
    )
    factor = update_gain * math.sqrt(max(FEATURES, OUTPUTS)) / divisor
    update = (factor[:, None, None] * polished).astype(jnp.bfloat16)
    return lax.all_gather(update, "dp", axis=0, tiled=True)


def solution(mesh):
    placed = (P("dp", "tensor", None),)
    return jax.shard_map(
        on_device, mesh=mesh, in_specs=placed, out_specs=P(None, "tensor", None), check_vma=False
    )
```

```python
import functools
import math

import jax
import jax.numpy as jnp
from jax import lax
from jax.experimental import pallas as pl
from jax.experimental.pallas import tpu as pltpu
from jax.sharding import PartitionSpec as P

FEATURES = 8192
OUTPUTS = 512
ITERS = 3

linear_term = 3.4445
cubic_term = -4.775
quintic_term = 2.0315
norm_floor = 1e-07
update_gain = 0.2

LANES = 128
SUBLANES = 8


def partners_of(group):
    return [partner for partner in (7, 3, 5, 6, 1, 2, 4) if partner < group]


def split(value):
    high = value.astype(jnp.bfloat16)
    low = (value - high.astype(jnp.float32)).astype(jnp.bfloat16)
    return high, low


def wide(value, axis):
    high, low = split(value)
    return jnp.concatenate([high, high, low] if axis == 1 else [high, low, high], axis=axis)


def dot(first, second, contract=(1, 0)):
    return lax.dot_general(
        first, second, (((contract[0],), (contract[1],)), ((), ())), preferred_element_type=jnp.float32
    )


def grid_pair(half):
    shape = (half, half)
    return lax.broadcasted_iota(jnp.int32, shape, 0), lax.broadcasted_iota(jnp.int32, shape, 1)


def member(group):
    return lax.rem(lax.axis_index("tensor"), group)


def gram_kernel(group, gradient_ref, *refs):
    chunks, (mixed, cross) = refs[:group], refs[group:]
    half = mixed.shape[0]
    rows = half // group
    high, low = split(gradient_ref[0])
    left = jnp.concatenate([high, high, low], axis=0)
    right = jnp.concatenate([high, low, high], axis=0)
    first = dot(left[:, :half], right[:, :half], (0, 0))
    cross[...] = dot(left[:, :half], right[:, half:], (0, 0))
    second = dot(left[:, half:], right[:, half:], (0, 0))
    row, column = grid_pair(half)
    mixed[...] = jnp.where(row <= column, first, second)
    diagonal = jnp.sum(jnp.where(row == column, second, 0.0), axis=0, keepdims=True)
    me = member(group)
    for slot, partner in enumerate([0] + partners_of(group)):
        start = pl.multiple_of((me ^ partner) * rows, rows)
        out = chunks[slot]
        at = 0
        for source in (cross, mixed):
            for lane in range(0, half, LANES):
                out[at : at + rows, :] = source[pl.ds(start, rows), lane : lane + LANES]
                at += rows
        for lane in range(0, half, LANES):
            out[at : at + SUBLANES, :] = jnp.broadcast_to(diagonal[:, lane : lane + LANES], (SUBLANES, LANES))
            at += SUBLANES


def update_kernel(group, gain, *refs):
    chunks = refs[:group]
    gradient_hbm, update_ref, mixed, cross, gradient, sem = refs[group:]
    copy = pltpu.make_async_copy(gradient_hbm.at[0], gradient, sem)
    copy.start()
    half = mixed.shape[0]
    rows = half // group
    me = member(group)
    for slot, partner in enumerate([0] + partners_of(group)):
        start = pl.multiple_of((me ^ partner) * rows, rows)
        source = chunks[slot]
        at = 0
        for target in (cross, mixed):
            for lane in range(0, half, LANES):
                target[pl.ds(start, rows), lane : lane + LANES] = source[at : at + rows, :]
                at += rows
    tiles = [chunks[0][at + i * SUBLANES : at + i * SUBLANES + 1, :] for i in range(half // LANES)]
    diagonal = jnp.concatenate(tiles, axis=1)
    row, column = grid_pair(half)
    packed = mixed[...]
    flipped = packed.T
    first = jnp.where(row <= column, packed, flipped)
    second = jnp.where(row > column, packed, flipped)
    on_diagonal = row == column
    second = jnp.where(on_diagonal, jnp.broadcast_to(diagonal, (half, half)), second)
    corner = cross[...]
    norm = jnp.sum(jnp.where(on_diagonal, first + second, 0.0), keepdims=True)
    divisor = jnp.sqrt(norm) + norm_floor
    scale = 1.0 / (divisor * divisor)
    gram = jnp.concatenate(
        [jnp.concatenate([first, corner], axis=1), jnp.concatenate([corner.T, second], axis=1)], axis=0
    )
    gram = gram * scale
    row, column = grid_pair(2 * half)
    identity = jnp.where(row == column, linear_term, 0.0)
    total = None
    for turn in range(ITERS):
        gram_left, gram_right = wide(gram, 1), wide(gram, 0)
        squared = dot(gram_left, gram_right)
        polynomial = identity + cubic_term * gram + quintic_term * squared
        polynomial_right = wide(polynomial, 0)
        total = polynomial if total is None else dot(wide(total, 1), polynomial_right)
        if turn + 1 < ITERS:
            gram = dot(wide(dot(gram_left, polynomial_right), 1), polynomial_right)
    copy.wait()
    polished = dot(wide(gradient[...], 1), wide(total, 0))
    update_ref[0] = ((gain / divisor) * polished).astype(jnp.bfloat16)


def on_device(mesh, gradient):
    size = mesh.shape["tensor"]
    group = min(8, size)
    assert size & (size - 1) == 0
    _, features, outputs = gradient.shape
    half = outputs // 2
    chunk = jax.ShapeDtypeStruct((2 * half // group * (half // LANES) + SUBLANES * (half // LANES), LANES), jnp.float32)
    vmem = pl.BlockSpec(memory_space=pltpu.VMEM)

    def swap(value, partner):
        return lax.ppermute(value, "tensor", [(i, i ^ partner) for i in range(size)])

    chunks = pl.pallas_call(
        functools.partial(gram_kernel, group),
        out_shape=[chunk] * group,
        in_specs=[vmem],
        out_specs=[vmem] * group,
        scratch_shapes=[pltpu.VMEM((half, half), jnp.float32)] * 2,
        name="gram",
    )(gradient)
    partners = partners_of(group)
    arrived = [swap(value, partner) for value, partner in zip(chunks[1:], partners)]
    owned = functools.reduce(jnp.add, arrived, chunks[0])
    step = group
    while step < size:
        owned = owned + swap(owned, step)
        step *= 2
    gathered = [owned] + [swap(owned, partner) for partner in partners]
    gain = update_gain * math.sqrt(max(FEATURES, OUTPUTS))
    update = pl.pallas_call(
        functools.partial(update_kernel, group, gain),
        out_shape=jax.ShapeDtypeStruct(gradient.shape, jnp.bfloat16),
        in_specs=[vmem] * group + [pl.BlockSpec(memory_space=pl.ANY)],
        out_specs=vmem,
        scratch_shapes=[
            pltpu.VMEM((half, half), jnp.float32),
            pltpu.VMEM((half, half), jnp.float32),
            pltpu.VMEM((features, outputs), jnp.float32),
            pltpu.SemaphoreType.DMA,
        ],
        name="update",
    )(*gathered, gradient)
    if mesh.shape["dp"] != 2:
        return lax.all_gather(update, "dp", axis=0, tiled=True)
    other = lax.ppermute(update, "dp", [(0, 1), (1, 0)])
    first = lax.axis_index("dp") == 0
    return jnp.where(first, jnp.concatenate([update, other]), jnp.concatenate([other, update]))


def solution(mesh):
    placed = (P("dp", "tensor", None),)
    return jax.shard_map(
        functools.partial(on_device, mesh), mesh=mesh, in_specs=placed, out_specs=P(None, "tensor", None), check_vma=False
    )
```

```python
import functools
import math

import jax
import jax.numpy as jnp
from jax import lax
from jax.experimental import pallas as pl
from jax.experimental.pallas import tpu as pltpu
from jax.sharding import PartitionSpec as P

FEATURES = 8192
OUTPUTS = 512
ITERS = 3

linear_term = 3.4445
cubic_term = -4.775
quintic_term = 2.0315
norm_floor = 1e-07
update_gain = 0.2

LANES = 128
GRAM_VMEM = 16 << 20
UPDATE_VMEM = 32 << 20
PLACE_VMEM = 4 << 20
SUBLANES = 8


def partners_of(group):
    return [partner for partner in (7, 3, 5, 6, 1, 2, 4) if partner < group]


def split(value):
    high = value.astype(jnp.bfloat16)
    low = (value - high.astype(jnp.float32)).astype(jnp.bfloat16)
    return high, low


def wide(value, axis):
    high, low = split(value)
    return jnp.concatenate([high, high, low] if axis == 1 else [high, low, high], axis=axis)


def dot(first, second, contract=(1, 0)):
    return lax.dot_general(
        first, second, (((contract[0],), (contract[1],)), ((), ())), preferred_element_type=jnp.float32
    )


def grid_pair(half):
    shape = (half, half)
    return lax.broadcasted_iota(jnp.int32, shape, 0), lax.broadcasted_iota(jnp.int32, shape, 1)


def member(group):
    return lax.rem(lax.axis_index("tensor"), group)


def gram_kernel(group, gradient_ref, *refs):
    chunks, (mixed, cross) = refs[:group], refs[group:]
    half = mixed.shape[0]
    rows = half // group
    high, low = split(gradient_ref[0])
    left = jnp.concatenate([high, high, low], axis=0)
    right = jnp.concatenate([high, low, high], axis=0)
    first = dot(left[:, :half], right[:, :half], (0, 0))
    cross[...] = dot(left[:, :half], right[:, half:], (0, 0))
    second = dot(left[:, half:], right[:, half:], (0, 0))
    row, column = grid_pair(half)
    mixed[...] = jnp.where(row <= column, first, second)
    diagonal = jnp.sum(jnp.where(row == column, second, 0.0), axis=0, keepdims=True)
    me = member(group)
    for slot, partner in enumerate([0] + partners_of(group)):
        start = pl.multiple_of((me ^ partner) * rows, rows)
        out = chunks[slot]
        at = 0
        for source in (cross, mixed):
            for lane in range(0, half, LANES):
                out[at : at + rows, :] = source[pl.ds(start, rows), lane : lane + LANES]
                at += rows
        for lane in range(0, half, LANES):
            out[at : at + SUBLANES, :] = jnp.broadcast_to(diagonal[:, lane : lane + LANES], (SUBLANES, LANES))
            at += SUBLANES


def update_kernel(group, gain, *refs):
    chunks = refs[:group]
    gradient_ref, update_ref, whole_hbm, mixed, cross, store_sem = refs[group:]
    half = mixed.shape[0]
    rows = half // group
    me = member(group)
    for slot, partner in enumerate([0] + partners_of(group)):
        start = pl.multiple_of((me ^ partner) * rows, rows)
        source = chunks[slot]
        at = 0
        for target in (cross, mixed):
            for lane in range(0, half, LANES):
                target[pl.ds(start, rows), lane : lane + LANES] = source[at : at + rows, :]
                at += rows
    tiles = [chunks[0][at + i * SUBLANES : at + i * SUBLANES + 1, :] for i in range(half // LANES)]
    diagonal = jnp.concatenate(tiles, axis=1)
    row, column = grid_pair(half)
    packed = mixed[...]
    flipped = packed.T
    first = jnp.where(row <= column, packed, flipped)
    second = jnp.where(row > column, packed, flipped)
    on_diagonal = row == column
    second = jnp.where(on_diagonal, jnp.broadcast_to(diagonal, (half, half)), second)
    corner = cross[...]
    norm = jnp.sum(jnp.where(on_diagonal, first + second, 0.0), keepdims=True)
    divisor = jnp.sqrt(norm) + norm_floor
    scale = 1.0 / (divisor * divisor)
    gram = jnp.concatenate(
        [jnp.concatenate([first, corner], axis=1), jnp.concatenate([corner.T, second], axis=1)], axis=0
    )
    gram = gram * scale
    row, column = grid_pair(2 * half)
    identity = jnp.where(row == column, linear_term, 0.0)
    total = None
    for turn in range(ITERS):
        gram_left, gram_right = wide(gram, 1), wide(gram, 0)
        squared = dot(gram_left, gram_right)
        polynomial = identity + cubic_term * gram + quintic_term * squared
        polynomial_right = wide(polynomial, 0)
        total = polynomial if total is None else dot(wide(total, 1), polynomial_right)
        if turn + 1 < ITERS:
            gram = dot(wide(dot(gram_left, polynomial_right), 1), polynomial_right)
    polished = dot(wide(gradient_ref[0], 1), wide(total, 0))
    update_ref[0] = ((gain / divisor) * polished).astype(jnp.bfloat16)
    store = pltpu.make_async_copy(update_ref.at[0], whole_hbm.at[lax.axis_index("dp")], store_sem)
    store.start()
    store.wait()


def place_kernel(other_ref, whole_in, whole_hbm, sem):
    del whole_in
    copy = pltpu.make_async_copy(other_ref.at[0], whole_hbm.at[1 - lax.axis_index("dp")], sem)
    copy.start()
    copy.wait()


def on_device(mesh, gradient):
    size = mesh.shape["tensor"]
    group = min(8, size)
    assert size & (size - 1) == 0
    _, features, outputs = gradient.shape
    half = outputs // 2
    chunk = jax.ShapeDtypeStruct((2 * half // group * (half // LANES) + SUBLANES * (half // LANES), LANES), jnp.float32)
    vmem = pl.BlockSpec(memory_space=pltpu.VMEM)
    anywhere = pl.BlockSpec(memory_space=pl.ANY)

    def swap(value, partner):
        return lax.ppermute(value, "tensor", [(i, i ^ partner) for i in range(size)])

    chunks = pl.pallas_call(
        functools.partial(gram_kernel, group),
        out_shape=[chunk] * group,
        in_specs=[vmem],
        out_specs=[vmem] * group,
        scratch_shapes=[pltpu.VMEM((half, half), jnp.float32)] * 2,
        compiler_params=pltpu.CompilerParams(vmem_limit_bytes=GRAM_VMEM),
        name="gram",
    )(gradient)
    partners = partners_of(group)
    arrived = [swap(value, partner) for value, partner in zip(chunks[1:], partners)]
    owned = functools.reduce(jnp.add, arrived, chunks[0])
    step = group
    while step < size:
        owned = owned + swap(owned, step)
        step *= 2
    gathered = [owned] + [swap(owned, partner) for partner in partners]
    gain = update_gain * math.sqrt(max(FEATURES, OUTPUTS))
    pairs = mesh.shape["dp"]
    whole = jax.ShapeDtypeStruct((pairs, features, outputs), jnp.bfloat16)
    update, placed = pl.pallas_call(
        functools.partial(update_kernel, group, gain),
        out_shape=[jax.ShapeDtypeStruct(gradient.shape, jnp.bfloat16), whole],
        in_specs=[vmem] * (group + 1),
        out_specs=[vmem, anywhere],
        scratch_shapes=[
            pltpu.VMEM((half, half), jnp.float32),
            pltpu.VMEM((half, half), jnp.float32),
            pltpu.SemaphoreType.DMA,
        ],
        compiler_params=pltpu.CompilerParams(vmem_limit_bytes=UPDATE_VMEM),
        name="update",
    )(*gathered, gradient)
    if pairs != 2:
        return lax.all_gather(update, "dp", axis=0, tiled=True)
    other = lax.ppermute(update, "dp", [(0, 1), (1, 0)])
    return pl.pallas_call(
        place_kernel,
        out_shape=whole,
        in_specs=[vmem, anywhere],
        out_specs=anywhere,
        scratch_shapes=[pltpu.SemaphoreType.DMA],
        input_output_aliases={1: 0},
        compiler_params=pltpu.CompilerParams(vmem_limit_bytes=PLACE_VMEM),
        name="place",
    )(other, placed)


def solution(mesh):
    placed = (P("dp", "tensor", None),)
    return jax.shard_map(
        functools.partial(on_device, mesh), mesh=mesh, in_specs=placed, out_specs=P(None, "tensor", None), check_vma=False
    )
```

```python
import functools
import math

import jax
import jax.numpy as jnp
from jax import lax
from jax.experimental import pallas as pl
from jax.experimental.pallas import tpu as pltpu
from jax.sharding import PartitionSpec as P

FEATURES = 8192
OUTPUTS = 512
ITERS = 3

linear_term = 3.4445
cubic_term = -4.775
quintic_term = 2.0315
norm_floor = 1e-07
update_gain = 0.2

LANES = 128
GRAM_VMEM = 16 << 20
UPDATE_VMEM = 32 << 20
PLACE_VMEM = 4 << 20
SUBLANES = 8


GROUP = 8
SOUTH = (3, 4, 2, 0)
NORTH = (7, 6, 5, 1)


def split(value):
    high = value.astype(jnp.bfloat16)
    low = (value - high.astype(jnp.float32)).astype(jnp.bfloat16)
    return high, low


def wide(value, axis):
    high, low = split(value)
    return jnp.concatenate([high, high, low] if axis == 1 else [high, low, high], axis=axis)


def dot(first, second, contract=(1, 0)):
    return lax.dot_general(
        first, second, (((contract[0],), (contract[1],)), ((), ())), preferred_element_type=jnp.float32
    )


def grid_pair(half):
    shape = (half, half)
    return lax.broadcasted_iota(jnp.int32, shape, 0), lax.broadcasted_iota(jnp.int32, shape, 1)


def block_starts(rows):
    me = lax.rem(lax.axis_index("tensor"), GROUP)
    north = lax.rem(lax.axis_index("dp"), 2) == 1
    own, other = [], []
    for first, second in zip(SOUTH, NORTH):
        own.append(pl.multiple_of((me ^ jnp.where(north, second, first)) * rows, rows))
        other.append(pl.multiple_of((me ^ jnp.where(north, first, second)) * rows, rows))
    return own, other


def gram_kernel(gradient_ref, *refs):
    slots = len(SOUTH)
    chunks, send, (mixed, cross) = refs[:slots], refs[slots], refs[slots + 1 :]
    half = mixed.shape[0]
    rows = half // GROUP
    size = chunks[0].shape[0]
    high, low = split(gradient_ref[0])
    left = jnp.concatenate([high, high, low], axis=0)
    right = jnp.concatenate([high, low, high], axis=0)
    first = dot(left[:, :half], right[:, :half], (0, 0))
    cross[...] = dot(left[:, :half], right[:, half:], (0, 0))
    second = dot(left[:, half:], right[:, half:], (0, 0))
    row, column = grid_pair(half)
    mixed[...] = jnp.where(row <= column, first, second)
    diagonal = jnp.sum(jnp.where(row == column, second, 0.0), axis=0, keepdims=True)
    which = lax.broadcasted_iota(jnp.int32, (SUBLANES, LANES), 0)
    tile = jnp.zeros((SUBLANES, LANES), jnp.float32)
    for index in range(half // LANES):
        part = diagonal[:, index * LANES : (index + 1) * LANES]
        tile = jnp.where(which == index, jnp.broadcast_to(part, (SUBLANES, LANES)), tile)

    def write(out, at, start):
        for source in (cross, mixed):
            for lane in range(0, half, LANES):
                out[at : at + rows, :] = source[pl.ds(start, rows), lane : lane + LANES]
                at += rows
        out[at : at + SUBLANES, :] = tile

    own, other = block_starts(rows)
    for slot in range(slots):
        write(send, slot * size, other[slot])
    for slot in range(slots):
        write(chunks[slot], 0, own[slot])


def update_kernel(gain, *refs):
    slots = len(SOUTH)
    own_chunks, other_chunks = refs[:slots], refs[slots : 2 * slots]
    gradient_ref, update_ref, whole_hbm, mixed, cross, store_sem = refs[2 * slots :]
    half = mixed.shape[0]
    rows = half // GROUP
    own, other = block_starts(rows)
    for source, start in zip((*own_chunks, *other_chunks), own + other):
        at = 0
        for target in (cross, mixed):
            for lane in range(0, half, LANES):
                target[pl.ds(start, rows), lane : lane + LANES] = source[at : at + rows, :]
                at += rows
    diagonal = jnp.concatenate([own_chunks[0][at + i : at + i + 1, :] for i in range(half // LANES)], axis=1)
    row, column = grid_pair(half)
    packed = mixed[...]
    flipped = packed.T
    first = jnp.where(row <= column, packed, flipped)
    second = jnp.where(row > column, packed, flipped)
    on_diagonal = row == column
    second = jnp.where(on_diagonal, jnp.broadcast_to(diagonal, (half, half)), second)
    corner = cross[...]
    norm = jnp.sum(jnp.where(on_diagonal, first + second, 0.0), keepdims=True)
    divisor = jnp.sqrt(norm) + norm_floor
    scale = 1.0 / (divisor * divisor)
    gram = jnp.concatenate(
        [jnp.concatenate([first, corner], axis=1), jnp.concatenate([corner.T, second], axis=1)], axis=0
    )
    gram = gram * scale
    row, column = grid_pair(2 * half)
    identity = jnp.where(row == column, linear_term, 0.0)
    total = None
    for turn in range(ITERS):
        gram_left, gram_right = wide(gram, 1), wide(gram, 0)
        squared = dot(gram_left, gram_right)
        polynomial = identity + cubic_term * gram + quintic_term * squared
        polynomial_right = wide(polynomial, 0)
        total = polynomial if total is None else dot(wide(total, 1), polynomial_right)
        if turn + 1 < ITERS:
            gram = dot(wide(dot(gram_left, polynomial_right), 1), polynomial_right)
    polished = dot(wide(gradient_ref[0], 1), wide(total, 0))
    update_ref[0] = ((gain / divisor) * polished).astype(jnp.bfloat16)
    store = pltpu.make_async_copy(update_ref.at[0], whole_hbm.at[lax.axis_index("dp")], store_sem)
    store.start()
    store.wait()


def place_kernel(other_ref, whole_in, whole_hbm, sem):
    del whole_in
    copy = pltpu.make_async_copy(other_ref.at[0], whole_hbm.at[1 - lax.axis_index("dp")], sem)
    copy.start()
    copy.wait()


def on_device(mesh, gradient):
    pairs, size = mesh.shape["dp"], mesh.shape["tensor"]
    assert pairs % 2 == 0 and size % GROUP == 0 and size & (size - 1) == 0
    _, features, outputs = gradient.shape
    half, slots = outputs // 2, len(SOUTH)
    assert half // LANES <= SUBLANES
    length = 2 * half // GROUP * (half // LANES) + SUBLANES
    chunk = jax.ShapeDtypeStruct((length, LANES), jnp.float32)
    vmem = pl.BlockSpec(memory_space=pltpu.VMEM)
    anywhere = pl.BlockSpec(memory_space=pl.ANY)

    def flip(value):
        return lax.ppermute(value, "dp", [(d, d ^ 1) for d in range(pairs)])

    def far(value, step):
        return lax.ppermute(value, "tensor", [(i, i ^ step) for i in range(size)])

    def near(value, slot):
        partner = (SOUTH[slot], NORTH[slot])
        moves = [(d * size + i, d * size + (i ^ partner[d % 2])) for d in range(pairs) for i in range(size)]
        return lax.ppermute(value, ("dp", "tensor"), moves)

    *own, send = pl.pallas_call(
        gram_kernel,
        out_shape=[chunk] * slots + [jax.ShapeDtypeStruct((slots * length, LANES), jnp.float32)],
        in_specs=[vmem],
        out_specs=[vmem] * (slots + 1),
        scratch_shapes=[pltpu.VMEM((half, half), jnp.float32)] * 2,
        compiler_params=pltpu.CompilerParams(vmem_limit_bytes=GRAM_VMEM),
        name="gram",
    )(gradient)
    held = flip(send)
    arrived = []
    for slot in range(slots):
        message = jnp.concatenate([own[slot], held[slot * length : (slot + 1) * length]])
        arrived.append(near(message, slot))
    partial = functools.reduce(jnp.add, arrived)
    mine = partial[:length] + flip(partial[length:])
    step = GROUP
    while step < size:
        mine = mine + far(mine, step)
        step *= 2
    both = jnp.concatenate([mine, flip(mine)])
    gathered = [near(both, slot) for slot in range(slots)]
    passed = [flip(value[length:]) for value in gathered]
    gain = update_gain * math.sqrt(max(FEATURES, OUTPUTS))
    whole = jax.ShapeDtypeStruct((pairs, features, outputs), jnp.bfloat16)
    update, placed = pl.pallas_call(
        functools.partial(update_kernel, gain),
        out_shape=[jax.ShapeDtypeStruct(gradient.shape, jnp.bfloat16), whole],
        in_specs=[vmem] * (2 * slots + 1),
        out_specs=[vmem, anywhere],
        scratch_shapes=[
            pltpu.VMEM((half, half), jnp.float32),
            pltpu.VMEM((half, half), jnp.float32),
            pltpu.SemaphoreType.DMA,
        ],
        compiler_params=pltpu.CompilerParams(vmem_limit_bytes=UPDATE_VMEM),
        name="update",
    )(*gathered, *passed, gradient)
    if pairs != 2:
        return lax.all_gather(update, "dp", axis=0, tiled=True)
    other = lax.ppermute(update, "dp", [(0, 1), (1, 0)])
    return pl.pallas_call(
        place_kernel,
        out_shape=whole,
        in_specs=[vmem, anywhere],
        out_specs=anywhere,
        scratch_shapes=[pltpu.SemaphoreType.DMA],
        input_output_aliases={1: 0},
        compiler_params=pltpu.CompilerParams(vmem_limit_bytes=PLACE_VMEM),
        name="place",
    )(other, placed)


def solution(mesh):
    placed = (P("dp", "tensor", None),)
    return jax.shard_map(
        functools.partial(on_device, mesh), mesh=mesh, in_specs=placed, out_specs=P(None, "tensor", None), check_vma=False
    )
```

```python
import functools
import math

import jax
import jax.numpy as jnp
from jax import lax
from jax.experimental import pallas as pl
from jax.experimental.pallas import tpu as pltpu
from jax.sharding import PartitionSpec as P

FEATURES = 8192
OUTPUTS = 512
ITERS = 3

linear_term = 3.4445
cubic_term = -4.775
quintic_term = 2.0315
norm_floor = 1e-07
update_gain = 0.2

LANES = 128
GRAM_VMEM = 16 << 20
UPDATE_VMEM = 32 << 20
PLACE_VMEM = 4 << 20
SUBLANES = 8


GROUP = 8
PARTNERS = (0, 7, 6, 5, 3, 4, 1, 2)


def split(value):
    high = value.astype(jnp.bfloat16)
    low = (value - high.astype(jnp.float32)).astype(jnp.bfloat16)
    return high, low


def wide(value, axis):
    high, low = split(value)
    return jnp.concatenate([high, high, low] if axis == 1 else [high, low, high], axis=axis)


def dot(first, second, contract=(1, 0)):
    return lax.dot_general(
        first, second, (((contract[0],), (contract[1],)), ((), ())), preferred_element_type=jnp.float32
    )


def grid_pair(half):
    shape = (half, half)
    return lax.broadcasted_iota(jnp.int32, shape, 0), lax.broadcasted_iota(jnp.int32, shape, 1)


def block_starts(rows):
    me = lax.rem(lax.axis_index("tensor"), GROUP)
    return [pl.multiple_of((me ^ partner) * rows, rows) for partner in PARTNERS]


def gram_kernel(gradient_ref, *refs):
    chunks, (mixed, cross) = refs[:GROUP], refs[GROUP:]
    half = mixed.shape[0]
    rows = half // GROUP
    high, low = split(gradient_ref[0])
    left = jnp.concatenate([high, high, low], axis=0)
    right = jnp.concatenate([high, low, high], axis=0)
    first = dot(left[:, :half], right[:, :half], (0, 0))
    cross[...] = dot(left[:, :half], right[:, half:], (0, 0))
    second = dot(left[:, half:], right[:, half:], (0, 0))
    row, column = grid_pair(half)
    mixed[...] = jnp.where(row <= column, first, second)
    diagonal = jnp.sum(jnp.where(row == column, second, 0.0), axis=0, keepdims=True)
    which = lax.broadcasted_iota(jnp.int32, (SUBLANES, LANES), 0)
    tile = jnp.zeros((SUBLANES, LANES), jnp.float32)
    for index in range(half // LANES):
        part = diagonal[:, index * LANES : (index + 1) * LANES]
        tile = jnp.where(which == index, jnp.broadcast_to(part, (SUBLANES, LANES)), tile)

    def write(out, at, start):
        for source in (cross, mixed):
            for lane in range(0, half, LANES):
                out[at : at + rows, :] = source[pl.ds(start, rows), lane : lane + LANES]
                at += rows
        out[at : at + SUBLANES, :] = tile

    for out, start in zip(chunks, block_starts(rows)):
        write(out, 0, start)


def update_kernel(gain, *refs):
    gathered, passed = refs[:GROUP], refs[GROUP : 2 * GROUP]
    gradient_ref, update_ref, whole_hbm, mixed, cross, store_sem = refs[2 * GROUP :]
    half = mixed.shape[0]
    rows = half // GROUP
    length = passed[0].shape[0]
    north = lax.rem(lax.axis_index("dp"), 2) == 1
    for direct, relayed, start in zip(gathered, passed, block_starts(rows)):
        block = jnp.where(north, direct[length:, :], relayed[...])
        at = 0
        for target in (cross, mixed):
            for lane in range(0, half, LANES):
                target[pl.ds(start, rows), lane : lane + LANES] = block[at : at + rows, :]
                at += rows
    diagonal = jnp.concatenate([block[at + i : at + i + 1, :] for i in range(half // LANES)], axis=1)
    row, column = grid_pair(half)
    packed = mixed[...]
    flipped = packed.T
    first = jnp.where(row <= column, packed, flipped)
    second = jnp.where(row > column, packed, flipped)
    on_diagonal = row == column
    second = jnp.where(on_diagonal, jnp.broadcast_to(diagonal, (half, half)), second)
    corner = cross[...]
    norm = jnp.sum(jnp.where(on_diagonal, first + second, 0.0), keepdims=True)
    divisor = jnp.sqrt(norm) + norm_floor
    scale = 1.0 / (divisor * divisor)
    gram = jnp.concatenate(
        [jnp.concatenate([first, corner], axis=1), jnp.concatenate([corner.T, second], axis=1)], axis=0
    )
    gram = gram * scale
    row, column = grid_pair(2 * half)
    identity = jnp.where(row == column, linear_term, 0.0)
    total = None
    for turn in range(ITERS):
        gram_left, gram_right = wide(gram, 1), wide(gram, 0)
        squared = dot(gram_left, gram_right)
        polynomial = identity + cubic_term * gram + quintic_term * squared
        polynomial_right = wide(polynomial, 0)
        total = polynomial if total is None else dot(wide(total, 1), polynomial_right)
        if turn + 1 < ITERS:
            gram = dot(wide(dot(gram_left, polynomial_right), 1), polynomial_right)
    polished = dot(wide(gradient_ref[0], 1), wide(total, 0))
    update_ref[0] = ((gain / divisor) * polished).astype(jnp.bfloat16)
    store = pltpu.make_async_copy(update_ref.at[0], whole_hbm.at[lax.axis_index("dp")], store_sem)
    store.start()
    store.wait()


def place_kernel(other_ref, whole_in, whole_hbm, sem):
    del whole_in
    copy = pltpu.make_async_copy(other_ref.at[0], whole_hbm.at[1 - lax.axis_index("dp")], sem)
    copy.start()
    copy.wait()


def on_device(mesh, gradient):
    pairs, size = mesh.shape["dp"], mesh.shape["tensor"]
    assert pairs % 2 == 0 and size % GROUP == 0 and size & (size - 1) == 0
    _, features, outputs = gradient.shape
    half = outputs // 2
    assert half // LANES <= SUBLANES
    length = 2 * half // GROUP * (half // LANES) + SUBLANES
    chunk = jax.ShapeDtypeStruct((length, LANES), jnp.float32)
    vmem = pl.BlockSpec(memory_space=pltpu.VMEM)
    anywhere = pl.BlockSpec(memory_space=pl.ANY)

    def flip(value):
        return lax.ppermute(value, "dp", [(d, d ^ 1) for d in range(pairs)])

    def chips(value, partner):
        moves = [(d * size + i, d * size + (i ^ partner if d % 2 else i)) for d in range(pairs) for i in range(size)]
        return lax.ppermute(value, ("dp", "tensor"), moves)

    chunks = pl.pallas_call(
        gram_kernel,
        out_shape=[chunk] * GROUP,
        in_specs=[vmem],
        out_specs=[vmem] * GROUP,
        scratch_shapes=[pltpu.VMEM((half, half), jnp.float32)] * 2,
        compiler_params=pltpu.CompilerParams(vmem_limit_bytes=GRAM_VMEM),
        name="gram",
    )(gradient)
    messages = [jnp.concatenate([flip(value), value]) for value in chunks]
    both = functools.reduce(jnp.add, [chips(value, k) for value, k in zip(messages[1:], PARTNERS[1:])], messages[0])
    step = GROUP
    while step < size:
        both = both + chips(both, step)
        step *= 2
    gathered = [chips(both, partner) for partner in reversed(PARTNERS[1:])]
    gathered = [both] + gathered[::-1]
    passed = [flip(value[:length]) for value in gathered]
    gain = update_gain * math.sqrt(max(FEATURES, OUTPUTS))
    whole = jax.ShapeDtypeStruct((pairs, features, outputs), jnp.bfloat16)
    update, placed = pl.pallas_call(
        functools.partial(update_kernel, gain),
        out_shape=[jax.ShapeDtypeStruct(gradient.shape, jnp.bfloat16), whole],
        in_specs=[vmem] * (2 * GROUP + 1),
        out_specs=[vmem, anywhere],
        scratch_shapes=[
            pltpu.VMEM((half, half), jnp.float32),
            pltpu.VMEM((half, half), jnp.float32),
            pltpu.SemaphoreType.DMA,
        ],
        compiler_params=pltpu.CompilerParams(vmem_limit_bytes=UPDATE_VMEM),
        name="update",
    )(*gathered, *passed, gradient)
    if pairs != 2:
        return lax.all_gather(update, "dp", axis=0, tiled=True)
    other = lax.ppermute(update, "dp", [(0, 1), (1, 0)])
    return pl.pallas_call(
        place_kernel,
        out_shape=whole,
        in_specs=[vmem, anywhere],
        out_specs=anywhere,
        scratch_shapes=[pltpu.SemaphoreType.DMA],
        input_output_aliases={1: 0},
        compiler_params=pltpu.CompilerParams(vmem_limit_bytes=PLACE_VMEM),
        name="place",
    )(other, placed)


def solution(mesh):
    placed = (P("dp", "tensor", None),)
    return jax.shard_map(
        functools.partial(on_device, mesh), mesh=mesh, in_specs=placed, out_specs=P(None, "tensor", None), check_vma=False
    )
```

```python
import functools
import math

import jax
import jax.numpy as jnp
from jax import lax
from jax.experimental import pallas as pl
from jax.experimental.pallas import tpu as pltpu
from jax.sharding import PartitionSpec as P

FEATURES = 8192
OUTPUTS = 512
ITERS = 3

linear_term = 3.4445
cubic_term = -4.775
quintic_term = 2.0315
norm_floor = 1e-07
update_gain = 0.2

LANES = 128
GRAM_VMEM = 16 << 20
UPDATE_VMEM = 32 << 20
PLACE_VMEM = 4 << 20
SUBLANES = 8


GROUP = 8
PARTNERS = (7, 3, 5, 6, 1, 2, 4, 0)


def split(value):
    high = value.astype(jnp.bfloat16)
    low = (value - high.astype(jnp.float32)).astype(jnp.bfloat16)
    return high, low


def wide(value, axis):
    high, low = split(value)
    return jnp.concatenate([high, high, low] if axis == 1 else [high, low, high], axis=axis)


def dot(first, second, contract=(1, 0)):
    return lax.dot_general(
        first, second, (((contract[0],), (contract[1],)), ((), ())), preferred_element_type=jnp.float32
    )


def grid_pair(half):
    shape = (half, half)
    return lax.broadcasted_iota(jnp.int32, shape, 0), lax.broadcasted_iota(jnp.int32, shape, 1)


def block_starts(rows):
    me = lax.rem(lax.axis_index("tensor"), GROUP)
    return [pl.multiple_of((me ^ partner) * rows, rows) for partner in PARTNERS]


def gram_kernel(gradient_ref, *refs):
    chunks, (mixed, cross) = refs[:GROUP], refs[GROUP:]
    half = mixed.shape[0]
    rows = half // GROUP
    high, low = split(gradient_ref[0])
    left = jnp.concatenate([high, high, low], axis=0)
    right = jnp.concatenate([high, low, high], axis=0)
    first = dot(left[:, :half], right[:, :half], (0, 0))
    cross[...] = dot(left[:, :half], right[:, half:], (0, 0))
    second = dot(left[:, half:], right[:, half:], (0, 0))
    row, column = grid_pair(half)
    mixed[...] = jnp.where(row <= column, first, second)
    diagonal = jnp.sum(jnp.where(row == column, second, 0.0), axis=0, keepdims=True)
    which = lax.broadcasted_iota(jnp.int32, (SUBLANES, LANES), 0)
    tile = jnp.zeros((SUBLANES, LANES), jnp.float32)
    for index in range(half // LANES):
        part = diagonal[:, index * LANES : (index + 1) * LANES]
        tile = jnp.where(which == index, jnp.broadcast_to(part, (SUBLANES, LANES)), tile)

    def write(out, at, start):
        for source in (cross, mixed):
            for lane in range(0, half, LANES):
                out[at : at + rows, :] = source[pl.ds(start, rows), lane : lane + LANES]
                at += rows
        out[at : at + SUBLANES, :] = tile

    for out, start in zip(chunks, block_starts(rows)):
        write(out, 0, start)


def update_kernel(gain, *refs):
    chunks = refs[:GROUP]
    gradient_ref, update_ref, whole_hbm, mixed, cross, store_sem = refs[GROUP:]
    half = mixed.shape[0]
    rows = half // GROUP
    for source, start in zip(chunks, block_starts(rows)):
        at = 0
        for target in (cross, mixed):
            for lane in range(0, half, LANES):
                target[pl.ds(start, rows), lane : lane + LANES] = source[at : at + rows, :]
                at += rows
    diagonal = jnp.concatenate([chunks[0][at + i : at + i + 1, :] for i in range(half // LANES)], axis=1)
    row, column = grid_pair(half)
    packed = mixed[...]
    flipped = packed.T
    first = jnp.where(row <= column, packed, flipped)
    second = jnp.where(row > column, packed, flipped)
    on_diagonal = row == column
    second = jnp.where(on_diagonal, jnp.broadcast_to(diagonal, (half, half)), second)
    corner = cross[...]
    norm = jnp.sum(jnp.where(on_diagonal, first + second, 0.0), keepdims=True)
    divisor = jnp.sqrt(norm) + norm_floor
    scale = 1.0 / (divisor * divisor)
    gram = jnp.concatenate(
        [jnp.concatenate([first, corner], axis=1), jnp.concatenate([corner.T, second], axis=1)], axis=0
    )
    gram = gram * scale
    row, column = grid_pair(2 * half)
    identity = jnp.where(row == column, linear_term, 0.0)
    total = None
    for turn in range(ITERS):
        gram_left, gram_right = wide(gram, 1), wide(gram, 0)
        squared = dot(gram_left, gram_right)
        polynomial = identity + cubic_term * gram + quintic_term * squared
        polynomial_right = wide(polynomial, 0)
        total = polynomial if total is None else dot(wide(total, 1), polynomial_right)
        if turn + 1 < ITERS:
            gram = dot(wide(dot(gram_left, polynomial_right), 1), polynomial_right)
    polished = dot(wide(gradient_ref[0], 1), wide(total, 0))
    update_ref[0] = ((gain / divisor) * polished).astype(jnp.bfloat16)
    store = pltpu.make_async_copy(update_ref.at[0], whole_hbm.at[lax.axis_index("dp")], store_sem)
    store.start()
    store.wait()


def place_kernel(other_ref, whole_in, whole_hbm, sem):
    del whole_in
    copy = pltpu.make_async_copy(other_ref.at[0], whole_hbm.at[1 - lax.axis_index("dp")], sem)
    copy.start()
    copy.wait()


def on_device(mesh, gradient):
    pairs, size = mesh.shape["dp"], mesh.shape["tensor"]
    assert pairs % 2 == 0 and size % GROUP == 0 and size & (size - 1) == 0
    _, features, outputs = gradient.shape
    half = outputs // 2
    assert half // LANES <= SUBLANES
    length = 2 * half // GROUP * (half // LANES) + SUBLANES
    chunk = jax.ShapeDtypeStruct((length, LANES), jnp.float32)
    vmem = pl.BlockSpec(memory_space=pltpu.VMEM)
    anywhere = pl.BlockSpec(memory_space=pl.ANY)

    def across(value, partner):
        moves = [(d * size + i, (d ^ 1) * size + (i ^ partner)) for d in range(pairs) for i in range(size)]
        return lax.ppermute(value, ("dp", "tensor"), moves)

    def far(value, step):
        return lax.ppermute(value, "tensor", [(i, i ^ step) for i in range(size)])

    chunks = pl.pallas_call(
        gram_kernel,
        out_shape=[chunk] * GROUP,
        in_specs=[vmem],
        out_specs=[vmem] * GROUP,
        scratch_shapes=[pltpu.VMEM((half, half), jnp.float32)] * 2,
        compiler_params=pltpu.CompilerParams(vmem_limit_bytes=GRAM_VMEM),
        name="gram",
    )(gradient)
    owned = functools.reduce(jnp.add, [across(value, partner) for value, partner in zip(chunks, PARTNERS)])
    step = GROUP
    while step < size:
        owned = owned + far(owned, step)
        step *= 2
    gathered = [across(owned, partner) for partner in reversed(PARTNERS)][::-1]
    gain = update_gain * math.sqrt(max(FEATURES, OUTPUTS))
    whole = jax.ShapeDtypeStruct((pairs, features, outputs), jnp.bfloat16)
    update, placed = pl.pallas_call(
        functools.partial(update_kernel, gain),
        out_shape=[jax.ShapeDtypeStruct(gradient.shape, jnp.bfloat16), whole],
        in_specs=[vmem] * (GROUP + 1),
        out_specs=[vmem, anywhere],
        scratch_shapes=[
            pltpu.VMEM((half, half), jnp.float32),
            pltpu.VMEM((half, half), jnp.float32),
            pltpu.SemaphoreType.DMA,
        ],
        compiler_params=pltpu.CompilerParams(vmem_limit_bytes=UPDATE_VMEM),
        name="update",
    )(*gathered, gradient)
    if pairs != 2:
        return lax.all_gather(update, "dp", axis=0, tiled=True)
    other = lax.ppermute(update, "dp", [(0, 1), (1, 0)])
    return pl.pallas_call(
        place_kernel,
        out_shape=whole,
        in_specs=[vmem, anywhere],
        out_specs=anywhere,
        scratch_shapes=[pltpu.SemaphoreType.DMA],
        input_output_aliases={1: 0},
        compiler_params=pltpu.CompilerParams(vmem_limit_bytes=PLACE_VMEM),
        name="place",
    )(other, placed)


def solution(mesh):
    placed = (P("dp", "tensor", None),)
    return jax.shard_map(
        functools.partial(on_device, mesh), mesh=mesh, in_specs=placed, out_specs=P(None, "tensor", None), check_vma=False
    )
```

```python
import functools
import math

import jax
import jax.numpy as jnp
from jax import lax
from jax.experimental import pallas as pl
from jax.experimental.pallas import tpu as pltpu
from jax.sharding import PartitionSpec as P

FEATURES = 8192
OUTPUTS = 512
ITERS = 3

linear_term = 3.4445
cubic_term = -4.775
quintic_term = 2.0315
norm_floor = 1e-07
update_gain = 0.2

LANES = 128
GRAM_VMEM = 16 << 20
UPDATE_VMEM = 32 << 20
PLACE_VMEM = 4 << 20
SUBLANES = 8


GROUP = 8
SOUTH = (3, 4, 2)
NORTH = (7, 6, 5)
DIRECT = 1


def split(value):
    high = value.astype(jnp.bfloat16)
    low = (value - high.astype(jnp.float32)).astype(jnp.bfloat16)
    return high, low


def wide(value, axis):
    high, low = split(value)
    return jnp.concatenate([high, high, low] if axis == 1 else [high, low, high], axis=axis)


def dot(first, second, contract=(1, 0)):
    return lax.dot_general(
        first, second, (((contract[0],), (contract[1],)), ((), ())), preferred_element_type=jnp.float32
    )


def grid_pair(half):
    shape = (half, half)
    return lax.broadcasted_iota(jnp.int32, shape, 0), lax.broadcasted_iota(jnp.int32, shape, 1)


def block_starts(rows):
    me = lax.rem(lax.axis_index("tensor"), GROUP)
    north = lax.rem(lax.axis_index("dp"), 2) == 1
    own = [jnp.where(north, second, first) for first, second in zip(SOUTH, NORTH)]
    other = [jnp.where(north, first, second) for first, second in zip(SOUTH, NORTH)]
    return [pl.multiple_of((me ^ partner) * rows, rows) for partner in (0, DIRECT, *own, *other)]


def gram_kernel(gradient_ref, *refs):
    singles = 2 + len(SOUTH)
    chunks, send, (mixed, cross) = refs[:singles], refs[singles], refs[singles + 1 :]
    half = mixed.shape[0]
    rows = half // GROUP
    size = chunks[0].shape[0]
    high, low = split(gradient_ref[0])
    left = jnp.concatenate([high, high, low], axis=0)
    right = jnp.concatenate([high, low, high], axis=0)
    first = dot(left[:, :half], right[:, :half], (0, 0))
    cross[...] = dot(left[:, :half], right[:, half:], (0, 0))
    second = dot(left[:, half:], right[:, half:], (0, 0))
    row, column = grid_pair(half)
    mixed[...] = jnp.where(row <= column, first, second)
    diagonal = jnp.sum(jnp.where(row == column, second, 0.0), axis=0, keepdims=True)
    which = lax.broadcasted_iota(jnp.int32, (SUBLANES, LANES), 0)
    tile = jnp.zeros((SUBLANES, LANES), jnp.float32)
    for index in range(half // LANES):
        part = diagonal[:, index * LANES : (index + 1) * LANES]
        tile = jnp.where(which == index, jnp.broadcast_to(part, (SUBLANES, LANES)), tile)

    def write(out, at, start):
        for source in (cross, mixed):
            for lane in range(0, half, LANES):
                out[at : at + rows, :] = source[pl.ds(start, rows), lane : lane + LANES]
                at += rows
        out[at : at + SUBLANES, :] = tile

    starts = block_starts(rows)
    for slot, start in enumerate(starts[singles:]):
        write(send, slot * size, start)
    for out, start in zip(chunks, starts):
        write(out, 0, start)


def update_kernel(gain, *refs):
    chunks = refs[:GROUP]
    gradient_ref, update_ref, whole_hbm, mixed, cross, store_sem = refs[GROUP:]
    half = mixed.shape[0]
    rows = half // GROUP
    starts = block_starts(rows)
    slots = len(SOUTH)
    order = [1, 0, *range(1 + slots, 1, -1), *range(1 + 2 * slots, 1 + slots, -1)]
    for source, index in zip(chunks, order):
        start = starts[index]
        at = 0
        for target in (cross, mixed):
            for lane in range(0, half, LANES):
                target[pl.ds(start, rows), lane : lane + LANES] = source[at : at + rows, :]
                at += rows
    diagonal = jnp.concatenate([chunks[0][at + i : at + i + 1, :] for i in range(half // LANES)], axis=1)
    row, column = grid_pair(half)
    packed = mixed[...]
    flipped = packed.T
    first = jnp.where(row <= column, packed, flipped)
    second = jnp.where(row > column, packed, flipped)
    on_diagonal = row == column
    second = jnp.where(on_diagonal, jnp.broadcast_to(diagonal, (half, half)), second)
    corner = cross[...]
    norm = jnp.sum(jnp.where(on_diagonal, first + second, 0.0), keepdims=True)
    divisor = jnp.sqrt(norm) + norm_floor
    scale = 1.0 / (divisor * divisor)
    gram = jnp.concatenate(
        [jnp.concatenate([first, corner], axis=1), jnp.concatenate([corner.T, second], axis=1)], axis=0
    )
    gram = gram * scale
    row, column = grid_pair(2 * half)
    identity = jnp.where(row == column, linear_term, 0.0)
    total = None
    for turn in range(ITERS):
        gram_left, gram_right = wide(gram, 1), wide(gram, 0)
        squared = dot(gram_left, gram_right)
        polynomial = identity + cubic_term * gram + quintic_term * squared
        polynomial_right = wide(polynomial, 0)
        total = polynomial if total is None else dot(wide(total, 1), polynomial_right)
        if turn + 1 < ITERS:
            gram = dot(wide(dot(gram_left, polynomial_right), 1), polynomial_right)
    polished = dot(wide(gradient_ref[0], 1), wide(total, 0))
    update_ref[0] = ((gain / divisor) * polished).astype(jnp.bfloat16)
    store = pltpu.make_async_copy(update_ref.at[0], whole_hbm.at[lax.axis_index("dp")], store_sem)
    store.start()
    store.wait()


def place_kernel(other_ref, whole_in, whole_hbm, sem):
    del whole_in
    copy = pltpu.make_async_copy(other_ref.at[0], whole_hbm.at[1 - lax.axis_index("dp")], sem)
    copy.start()
    copy.wait()


def on_device(mesh, gradient):
    pairs, size = mesh.shape["dp"], mesh.shape["tensor"]
    assert pairs % 2 == 0 and size % GROUP == 0 and size & (size - 1) == 0
    _, features, outputs = gradient.shape
    half, slots = outputs // 2, len(SOUTH)
    assert half // LANES <= SUBLANES
    length = 2 * half // GROUP * (half // LANES) + SUBLANES
    chunk = jax.ShapeDtypeStruct((length, LANES), jnp.float32)
    vmem = pl.BlockSpec(memory_space=pltpu.VMEM)
    anywhere = pl.BlockSpec(memory_space=pl.ANY)

    def flip(value):
        return lax.ppermute(value, "dp", [(d, d ^ 1) for d in range(pairs)])

    def far(value, step):
        return lax.ppermute(value, "tensor", [(i, i ^ step) for i in range(size)])

    def near(value, slot):
        partner = (SOUTH[slot], NORTH[slot])
        moves = [(d * size + i, d * size + (i ^ partner[d % 2])) for d in range(pairs) for i in range(size)]
        return lax.ppermute(value, ("dp", "tensor"), moves)

    keep, direct, *own, send = pl.pallas_call(
        gram_kernel,
        out_shape=[chunk] * (2 + slots) + [jax.ShapeDtypeStruct((slots * length, LANES), jnp.float32)],
        in_specs=[vmem],
        out_specs=[vmem] * (3 + slots),
        scratch_shapes=[pltpu.VMEM((half, half), jnp.float32)] * 2,
        compiler_params=pltpu.CompilerParams(vmem_limit_bytes=GRAM_VMEM),
        name="gram",
    )(gradient)
    held = flip(send)
    mine = keep + far(direct, DIRECT)
    arrived = []
    for slot in range(slots):
        message = jnp.concatenate([own[slot], held[slot * length : (slot + 1) * length]])
        arrived.append(near(message, slot))
    partial = functools.reduce(jnp.add, arrived)
    mine = mine + partial[:length] + flip(partial[length:])
    step = GROUP
    while step < size:
        mine = mine + far(mine, step)
        step *= 2
    both = jnp.concatenate([mine, flip(mine)])
    direct = far(mine, DIRECT)
    gathered = [near(both, slot) for slot in range(slots)][::-1]
    passed = [flip(value[length:]) for value in gathered]
    gain = update_gain * math.sqrt(max(FEATURES, OUTPUTS))
    whole = jax.ShapeDtypeStruct((pairs, features, outputs), jnp.bfloat16)
    update, placed = pl.pallas_call(
        functools.partial(update_kernel, gain),
        out_shape=[jax.ShapeDtypeStruct(gradient.shape, jnp.bfloat16), whole],
        in_specs=[vmem] * (GROUP + 1),
        out_specs=[vmem, anywhere],
        scratch_shapes=[
            pltpu.VMEM((half, half), jnp.float32),
            pltpu.VMEM((half, half), jnp.float32),
            pltpu.SemaphoreType.DMA,
        ],
        compiler_params=pltpu.CompilerParams(vmem_limit_bytes=UPDATE_VMEM),
        name="update",
    )(direct, mine, *gathered, *passed, gradient)
    if pairs != 2:
        return lax.all_gather(update, "dp", axis=0, tiled=True)
    other = lax.ppermute(update, "dp", [(0, 1), (1, 0)])
    return pl.pallas_call(
        place_kernel,
        out_shape=whole,
        in_specs=[vmem, anywhere],
        out_specs=anywhere,
        scratch_shapes=[pltpu.SemaphoreType.DMA],
        input_output_aliases={1: 0},
        compiler_params=pltpu.CompilerParams(vmem_limit_bytes=PLACE_VMEM),
        name="place",
    )(other, placed)


def solution(mesh):
    placed = (P("dp", "tensor", None),)
    return jax.shard_map(
        functools.partial(on_device, mesh), mesh=mesh, in_specs=placed, out_specs=P(None, "tensor", None), check_vma=False
    )
```

```python
import functools
import math

import jax
import jax.numpy as jnp
from jax import lax
from jax.experimental import pallas as pl
from jax.experimental.pallas import tpu as pltpu
from jax.sharding import PartitionSpec as P

FEATURES = 8192
OUTPUTS = 512
ITERS = 3

linear_term = 3.4445
cubic_term = -4.775
quintic_term = 2.0315
norm_floor = 1e-07
update_gain = 0.2

LANES = 128
GRAM_VMEM = 16 << 20
UPDATE_VMEM = 32 << 20
PLACE_VMEM = 4 << 20
SUBLANES = 8


GROUP = 8
SOUTH = (3, 4, 2)
NORTH = (7, 6, 5)
DIRECT = 1


def split(value):
    high = value.astype(jnp.bfloat16)
    low = (value - high.astype(jnp.float32)).astype(jnp.bfloat16)
    return high, low


def wide(value, axis):
    high, low = split(value)
    return jnp.concatenate([high, high, low] if axis == 1 else [high, low, high], axis=axis)


def dot(first, second, contract=(1, 0)):
    return lax.dot_general(
        first, second, (((contract[0],), (contract[1],)), ((), ())), preferred_element_type=jnp.float32
    )


class Factor:
    def __init__(self, blocks):
        (high_a, low_a), (high_b, low_b), (high_c, low_c) = [split(block) for block in blocks]
        turned_high, turned_low = high_b.T, low_b.T
        rows = [((high_a, high_b), (low_a, low_b)), ((turned_high, high_c), (turned_low, low_c))]
        columns = [((high_a, turned_high), (low_a, turned_low)), ((high_b, high_c), (low_b, low_c))]
        self.left = [jnp.concatenate([*high, *high, *low], axis=1) for high, low in rows]
        self.right = [jnp.concatenate([*high, *low, *high], axis=0) for high, low in columns]

    def times(self, other):
        return [dot(self.left[i], other.right[j]) for i, j in ((0, 0), (0, 1), (1, 1))]


def grid_pair(half):
    shape = (half, half)
    return lax.broadcasted_iota(jnp.int32, shape, 0), lax.broadcasted_iota(jnp.int32, shape, 1)


def block_starts(rows):
    me = lax.rem(lax.axis_index("tensor"), GROUP)
    north = lax.rem(lax.axis_index("dp"), 2) == 1
    own = [jnp.where(north, second, first) for first, second in zip(SOUTH, NORTH)]
    other = [jnp.where(north, first, second) for first, second in zip(SOUTH, NORTH)]
    return [pl.multiple_of((me ^ partner) * rows, rows) for partner in (0, DIRECT, *own, *other)]


def gram_kernel(gradient_ref, *refs):
    singles = 2 + len(SOUTH)
    chunks, send, (mixed, cross) = refs[:singles], refs[singles], refs[singles + 1 :]
    half = mixed.shape[0]
    rows = half // GROUP
    size = chunks[0].shape[0]
    high, low = split(gradient_ref[0])
    left = jnp.concatenate([high, high, low], axis=0)
    right = jnp.concatenate([high, low, high], axis=0)
    first = dot(left[:, :half], right[:, :half], (0, 0))
    cross[...] = dot(left[:, :half], right[:, half:], (0, 0))
    second = dot(left[:, half:], right[:, half:], (0, 0))
    row, column = grid_pair(half)
    mixed[...] = jnp.where(row <= column, first, second)
    diagonal = jnp.sum(jnp.where(row == column, second, 0.0), axis=0, keepdims=True)
    which = lax.broadcasted_iota(jnp.int32, (SUBLANES, LANES), 0)
    tile = jnp.zeros((SUBLANES, LANES), jnp.float32)
    for index in range(half // LANES):
        part = diagonal[:, index * LANES : (index + 1) * LANES]
        tile = jnp.where(which == index, jnp.broadcast_to(part, (SUBLANES, LANES)), tile)

    def write(out, at, start):
        for source in (cross, mixed):
            for lane in range(0, half, LANES):
                out[at : at + rows, :] = source[pl.ds(start, rows), lane : lane + LANES]
                at += rows
        out[at : at + SUBLANES, :] = tile

    starts = block_starts(rows)
    for slot, start in enumerate(starts[singles:]):
        write(send, slot * size, start)
    for out, start in zip(chunks, starts):
        write(out, 0, start)


def update_kernel(gain, *refs):
    chunks = refs[:GROUP]
    gradient_ref, update_ref, whole_hbm, mixed, cross, store_sem = refs[GROUP:]
    half = mixed.shape[0]
    rows = half // GROUP
    starts = block_starts(rows)
    slots = len(SOUTH)
    order = [1, 0, *range(1 + slots, 1, -1), *range(1 + 2 * slots, 1 + slots, -1)]
    for source, index in zip(chunks, order):
        start = starts[index]
        at = 0
        for target in (cross, mixed):
            for lane in range(0, half, LANES):
                target[pl.ds(start, rows), lane : lane + LANES] = source[at : at + rows, :]
                at += rows
    diagonal = jnp.concatenate([chunks[0][at + i : at + i + 1, :] for i in range(half // LANES)], axis=1)
    row, column = grid_pair(half)
    on_diagonal = row == column
    packed = mixed[...]
    flipped = packed.T
    first = jnp.where(row <= column, packed, flipped)
    second = jnp.where(row > column, packed, flipped)
    second = jnp.where(on_diagonal, jnp.broadcast_to(diagonal, (half, half)), second)
    norm = jnp.sum(jnp.where(on_diagonal, first + second, 0.0), keepdims=True)
    divisor = jnp.sqrt(norm) + norm_floor
    scale = 1.0 / (divisor * divisor)
    gram = (first * scale, cross[...] * scale, second * scale)
    identity = jnp.where(on_diagonal, linear_term, 0.0)
    total = None
    for turn in range(ITERS):
        factor = Factor(gram)
        squared = factor.times(factor)
        polynomial = [cubic_term * g + quintic_term * q for g, q in zip(gram, squared)]
        polynomial = Factor((identity + polynomial[0], polynomial[1], identity + polynomial[2]))
        total = polynomial if total is None else Factor(total.times(polynomial))
        if turn + 1 < ITERS:
            gram = Factor(factor.times(polynomial)).times(polynomial)
    left = wide(gradient_ref[0], 1)
    for index in range(2):
        polished = dot(left, total.right[index])
        columns = slice(index * half, (index + 1) * half)
        update_ref[0, :, columns] = ((gain / divisor) * polished).astype(jnp.bfloat16)
    store = pltpu.make_async_copy(update_ref.at[0], whole_hbm.at[lax.axis_index("dp")], store_sem)
    store.start()
    store.wait()


def place_kernel(other_ref, whole_in, whole_hbm, sem):
    del whole_in
    copy = pltpu.make_async_copy(other_ref.at[0], whole_hbm.at[1 - lax.axis_index("dp")], sem)
    copy.start()
    copy.wait()


def on_device(mesh, gradient):
    pairs, size = mesh.shape["dp"], mesh.shape["tensor"]
    assert pairs % 2 == 0 and size % GROUP == 0 and size & (size - 1) == 0
    _, features, outputs = gradient.shape
    half, slots = outputs // 2, len(SOUTH)
    assert half // LANES <= SUBLANES
    length = 2 * half // GROUP * (half // LANES) + SUBLANES
    chunk = jax.ShapeDtypeStruct((length, LANES), jnp.float32)
    vmem = pl.BlockSpec(memory_space=pltpu.VMEM)
    anywhere = pl.BlockSpec(memory_space=pl.ANY)

    def flip(value):
        return lax.ppermute(value, "dp", [(d, d ^ 1) for d in range(pairs)])

    def far(value, step):
        return lax.ppermute(value, "tensor", [(i, i ^ step) for i in range(size)])

    def near(value, slot):
        partner = (SOUTH[slot], NORTH[slot])
        moves = [(d * size + i, d * size + (i ^ partner[d % 2])) for d in range(pairs) for i in range(size)]
        return lax.ppermute(value, ("dp", "tensor"), moves)

    keep, direct, *own, send = pl.pallas_call(
        gram_kernel,
        out_shape=[chunk] * (2 + slots) + [jax.ShapeDtypeStruct((slots * length, LANES), jnp.float32)],
        in_specs=[vmem],
        out_specs=[vmem] * (3 + slots),
        scratch_shapes=[pltpu.VMEM((half, half), jnp.float32)] * 2,
        compiler_params=pltpu.CompilerParams(vmem_limit_bytes=GRAM_VMEM),
        name="gram",
    )(gradient)
    held = flip(send)
    mine = keep + far(direct, DIRECT)
    arrived = []
    for slot in range(slots):
        message = jnp.concatenate([own[slot], held[slot * length : (slot + 1) * length]])
        arrived.append(near(message, slot))
    partial = functools.reduce(jnp.add, arrived)
    mine = mine + partial[:length] + flip(partial[length:])
    step = GROUP
    while step < size:
        mine = mine + far(mine, step)
        step *= 2
    both = jnp.concatenate([mine, flip(mine)])
    direct = far(mine, DIRECT)
    gathered = [near(both, slot) for slot in range(slots)][::-1]
    passed = [flip(value[length:]) for value in gathered]
    gain = update_gain * math.sqrt(max(FEATURES, OUTPUTS))
    whole = jax.ShapeDtypeStruct((pairs, features, outputs), jnp.bfloat16)
    update, placed = pl.pallas_call(
        functools.partial(update_kernel, gain),
        out_shape=[jax.ShapeDtypeStruct(gradient.shape, jnp.bfloat16), whole],
        in_specs=[vmem] * (GROUP + 1),
        out_specs=[vmem, anywhere],
        scratch_shapes=[
            pltpu.VMEM((half, half), jnp.float32),
            pltpu.VMEM((half, half), jnp.float32),
            pltpu.SemaphoreType.DMA,
        ],
        compiler_params=pltpu.CompilerParams(vmem_limit_bytes=UPDATE_VMEM),
        name="update",
    )(direct, mine, *gathered, *passed, gradient)
    if pairs != 2:
        return lax.all_gather(update, "dp", axis=0, tiled=True)
    other = lax.ppermute(update, "dp", [(0, 1), (1, 0)])
    return pl.pallas_call(
        place_kernel,
        out_shape=whole,
        in_specs=[vmem, anywhere],
        out_specs=anywhere,
        scratch_shapes=[pltpu.SemaphoreType.DMA],
        input_output_aliases={1: 0},
        compiler_params=pltpu.CompilerParams(vmem_limit_bytes=PLACE_VMEM),
        name="place",
    )(other, placed)


def solution(mesh):
    placed = (P("dp", "tensor", None),)
    return jax.shard_map(
        functools.partial(on_device, mesh), mesh=mesh, in_specs=placed, out_specs=P(None, "tensor", None), check_vma=False
    )
```

```python
import functools
import math

import jax
import jax.numpy as jnp
from jax import lax
from jax.experimental import pallas as pl
from jax.experimental.pallas import tpu as pltpu
from jax.sharding import PartitionSpec as P

FEATURES = 8192
OUTPUTS = 512
ITERS = 3

linear_term = 3.4445
cubic_term = -4.775
quintic_term = 2.0315
norm_floor = 1e-07
update_gain = 0.2

LANES = 128
GRAM_VMEM = 16 << 20
UPDATE_VMEM = 32 << 20
PLACE_COST = 1 << 20
PLACE_VMEM = 4 << 20
SUBLANES = 8


GROUP = 8
PARTNERS = (0, 7, 6, 5, 3, 4, 2, 1)
BACK = (1, 2, 4, 3, 5, 6, 7)


def split(value):
    high = value.astype(jnp.bfloat16)
    low = (value - high.astype(jnp.float32)).astype(jnp.bfloat16)
    return high, low


def wide(value, axis):
    high, low = split(value)
    return jnp.concatenate([high, high, low] if axis == 1 else [high, low, high], axis=axis)


def dot(first, second, contract=(1, 0)):
    return lax.dot_general(
        first, second, (((contract[0],), (contract[1],)), ((), ())), preferred_element_type=jnp.float32
    )


class Factor:
    def __init__(self, blocks):
        (high_a, low_a), (high_b, low_b), (high_c, low_c) = [split(block) for block in blocks]
        turned_high, turned_low = high_b.T, low_b.T
        rows = [((high_a, high_b), (low_a, low_b)), ((turned_high, high_c), (turned_low, low_c))]
        columns = [((high_a, turned_high), (low_a, turned_low)), ((high_b, high_c), (low_b, low_c))]
        self.left = [jnp.concatenate([*high, *high, *low], axis=1) for high, low in rows]
        self.right = [jnp.concatenate([*high, *low, *high], axis=0) for high, low in columns]

    def times(self, other):
        return [dot(self.left[i], other.right[j]) for i, j in ((0, 0), (0, 1), (1, 1))]


def grid_pair(half):
    shape = (half, half)
    return lax.broadcasted_iota(jnp.int32, shape, 0), lax.broadcasted_iota(jnp.int32, shape, 1)


def block_starts(rows, order):
    me = lax.rem(lax.axis_index("tensor"), GROUP)
    return [pl.multiple_of((me ^ partner) * rows, rows) for partner in order]


def gram_kernel(gradient_ref, *refs):
    chunks, (mixed, cross) = refs[:GROUP], refs[GROUP:]
    half = mixed.shape[0]
    rows = half // GROUP
    high, low = split(gradient_ref[0])
    left = jnp.concatenate([high, high, low], axis=0)
    right = jnp.concatenate([high, low, high], axis=0)
    first = dot(left[:, :half], right[:, :half], (0, 0))
    cross[...] = dot(left[:, :half], right[:, half:], (0, 0))
    second = dot(left[:, half:], right[:, half:], (0, 0))
    row, column = grid_pair(half)
    mixed[...] = jnp.where(row <= column, first, second)
    diagonal = jnp.sum(jnp.where(row == column, second, 0.0), axis=0, keepdims=True)
    which = lax.broadcasted_iota(jnp.int32, (SUBLANES, LANES), 0)
    tile = jnp.zeros((SUBLANES, LANES), jnp.float32)
    for index in range(half // LANES):
        part = diagonal[:, index * LANES : (index + 1) * LANES]
        tile = jnp.where(which == index, jnp.broadcast_to(part, (SUBLANES, LANES)), tile)

    def write(out, at, start):
        for source in (cross, mixed):
            for lane in range(0, half, LANES):
                out[at : at + rows, :] = source[pl.ds(start, rows), lane : lane + LANES]
                at += rows
        out[at : at + SUBLANES, :] = tile

    for out, start in zip(chunks, block_starts(rows, PARTNERS)):
        write(out, 0, start)


def update_kernel(gain, *refs):
    chunks = refs[:GROUP]
    gradient_ref, update_ref, mixed, cross = refs[GROUP:]
    half = mixed.shape[0]
    rows = half // GROUP
    for source, start in zip(chunks, block_starts(rows, (0, *BACK))):
        at = 0
        for target in (cross, mixed):
            for lane in range(0, half, LANES):
                target[pl.ds(start, rows), lane : lane + LANES] = source[at : at + rows, :]
                at += rows
    diagonal = jnp.concatenate([chunks[0][at + i : at + i + 1, :] for i in range(half // LANES)], axis=1)
    row, column = grid_pair(half)
    on_diagonal = row == column
    packed = mixed[...]
    flipped = packed.T
    first = jnp.where(row <= column, packed, flipped)
    second = jnp.where(row > column, packed, flipped)
    second = jnp.where(on_diagonal, jnp.broadcast_to(diagonal, (half, half)), second)
    norm = jnp.sum(jnp.where(on_diagonal, first + second, 0.0), keepdims=True)
    divisor = jnp.sqrt(norm) + norm_floor
    scale = 1.0 / (divisor * divisor)
    gram = (first * scale, cross[...] * scale, second * scale)
    identity = jnp.where(on_diagonal, linear_term, 0.0)
    total = None
    for turn in range(ITERS):
        factor = Factor(gram)
        squared = factor.times(factor)
        polynomial = [cubic_term * g + quintic_term * q for g, q in zip(gram, squared)]
        polynomial = Factor((identity + polynomial[0], polynomial[1], identity + polynomial[2]))
        total = polynomial if total is None else Factor(total.times(polynomial))
        if turn + 1 < ITERS:
            gram = Factor(factor.times(polynomial)).times(polynomial)
    left = wide(gradient_ref[0], 1)
    for index in range(2):
        polished = dot(left, total.right[index])
        columns = slice(index * half, (index + 1) * half)
        update_ref[0, :, columns] = ((gain / divisor) * polished).astype(jnp.bfloat16)


def place_kernel(flipped, value_ref, *refs):
    whole_hbm, sem = refs[-2:]
    index = lax.axis_index("dp")
    copy = pltpu.make_async_copy(value_ref.at[0], whole_hbm.at[1 - index if flipped else index], sem)
    copy.start()
    copy.wait()


def on_device(mesh, gradient):
    pairs, size = mesh.shape["dp"], mesh.shape["tensor"]
    assert pairs % 2 == 0 and size % GROUP == 0 and size & (size - 1) == 0
    _, features, outputs = gradient.shape
    half = outputs // 2
    assert half // LANES <= SUBLANES
    length = 2 * half // GROUP * (half // LANES) + SUBLANES
    chunk = jax.ShapeDtypeStruct((length, LANES), jnp.float32)
    vmem = pl.BlockSpec(memory_space=pltpu.VMEM)
    anywhere = pl.BlockSpec(memory_space=pl.ANY)

    def swap(value, partner):
        return lax.ppermute(value, "tensor", [(i, i ^ partner) for i in range(size)])

    chunks = pl.pallas_call(
        gram_kernel,
        out_shape=[chunk] * GROUP,
        in_specs=[vmem],
        out_specs=[vmem] * GROUP,
        scratch_shapes=[pltpu.VMEM((half, half), jnp.float32)] * 2,
        compiler_params=pltpu.CompilerParams(vmem_limit_bytes=GRAM_VMEM),
        name="gram",
    )(gradient)
    owned = functools.reduce(jnp.add, [swap(value, k) for value, k in zip(chunks[1:], PARTNERS[1:])], chunks[0])
    step = GROUP
    while step < size:
        owned = owned + swap(owned, step)
        step *= 2
    gathered = [owned] + [swap(owned, partner) for partner in BACK]
    gain = update_gain * math.sqrt(max(FEATURES, OUTPUTS))
    update = pl.pallas_call(
        functools.partial(update_kernel, gain),
        out_shape=jax.ShapeDtypeStruct(gradient.shape, jnp.bfloat16),
        in_specs=[vmem] * (GROUP + 1),
        out_specs=vmem,
        scratch_shapes=[pltpu.VMEM((half, half), jnp.float32)] * 2,
        compiler_params=pltpu.CompilerParams(vmem_limit_bytes=UPDATE_VMEM),
        name="update",
    )(*gathered, gradient)
    if pairs != 2:
        return lax.all_gather(update, "dp", axis=0, tiled=True)

    def place(flipped, *operands):
        return pl.pallas_call(
            functools.partial(place_kernel, flipped),
            out_shape=jax.ShapeDtypeStruct((pairs, features, outputs), jnp.bfloat16),
            in_specs=[vmem, anywhere][: len(operands)],
            out_specs=anywhere,
            scratch_shapes=[pltpu.SemaphoreType.DMA],
            input_output_aliases={1: 0} if flipped else {},
            compiler_params=pltpu.CompilerParams(vmem_limit_bytes=PLACE_VMEM),
            cost_estimate=pl.CostEstimate(flops=PLACE_COST, bytes_accessed=2 * features * outputs, transcendentals=0),
            name="place",
        )(*operands)

    other = lax.ppermute(update, "dp", [(0, 1), (1, 0)])
    return place(True, other, place(False, update))


def solution(mesh):
    placed = (P("dp", "tensor", None),)
    return jax.shard_map(
        functools.partial(on_device, mesh), mesh=mesh, in_specs=placed, out_specs=P(None, "tensor", None), check_vma=False
    )
```

```python
import functools
import math

import jax
import jax.numpy as jnp
from jax import lax
from jax.experimental import pallas as pl
from jax.experimental.pallas import tpu as pltpu
from jax.sharding import PartitionSpec as P

FEATURES = 8192
OUTPUTS = 512
ITERS = 3

linear_term = 3.4445
cubic_term = -4.775
quintic_term = 2.0315
norm_floor = 1e-07
update_gain = 0.2

LANES = 128
GRAM_VMEM = 16 << 20
UPDATE_VMEM = 32 << 20
PLACE_COST = 1 << 20
PLACE_VMEM = 4 << 20
SUBLANES = 8


GROUP = 8
PARTNERS = (0, 7, 6, 5, 3, 4, 2, 1)
RELAY = 4
LONE = (3, 7)
TWICE = (2, 1)
BLOCKS = (0, *[block for partner in TWICE for block in (partner, partner ^ RELAY)], *LONE, RELAY)


def split(value):
    high = value.astype(jnp.bfloat16)
    low = (value - high.astype(jnp.float32)).astype(jnp.bfloat16)
    return high, low


def wide(value, axis):
    high, low = split(value)
    return jnp.concatenate([high, high, low] if axis == 1 else [high, low, high], axis=axis)


def dot(first, second, contract=(1, 0)):
    return lax.dot_general(
        first, second, (((contract[0],), (contract[1],)), ((), ())), preferred_element_type=jnp.float32
    )


class Factor:
    def __init__(self, blocks):
        (high_a, low_a), (high_b, low_b), (high_c, low_c) = [split(block) for block in blocks]
        turned_high, turned_low = high_b.T, low_b.T
        rows = [((high_a, high_b), (low_a, low_b)), ((turned_high, high_c), (turned_low, low_c))]
        columns = [((high_a, turned_high), (low_a, turned_low)), ((high_b, high_c), (low_b, low_c))]
        self.left = [jnp.concatenate([*high, *high, *low], axis=1) for high, low in rows]
        self.right = [jnp.concatenate([*high, *low, *high], axis=0) for high, low in columns]

    def times(self, other):
        return [dot(self.left[i], other.right[j]) for i, j in ((0, 0), (0, 1), (1, 1))]


def grid_pair(half):
    shape = (half, half)
    return lax.broadcasted_iota(jnp.int32, shape, 0), lax.broadcasted_iota(jnp.int32, shape, 1)


def block_starts(rows, order):
    me = lax.rem(lax.axis_index("tensor"), GROUP)
    return [pl.multiple_of((me ^ partner) * rows, rows) for partner in order]


def gram_kernel(gradient_ref, *refs):
    chunks, (mixed, cross) = refs[:GROUP], refs[GROUP:]
    half = mixed.shape[0]
    rows = half // GROUP
    high, low = split(gradient_ref[0])
    left = jnp.concatenate([high, high, low], axis=0)
    right = jnp.concatenate([high, low, high], axis=0)
    first = dot(left[:, :half], right[:, :half], (0, 0))
    cross[...] = dot(left[:, :half], right[:, half:], (0, 0))
    second = dot(left[:, half:], right[:, half:], (0, 0))
    row, column = grid_pair(half)
    mixed[...] = jnp.where(row <= column, first, second)
    diagonal = jnp.sum(jnp.where(row == column, second, 0.0), axis=0, keepdims=True)
    which = lax.broadcasted_iota(jnp.int32, (SUBLANES, LANES), 0)
    tile = jnp.zeros((SUBLANES, LANES), jnp.float32)
    for index in range(half // LANES):
        part = diagonal[:, index * LANES : (index + 1) * LANES]
        tile = jnp.where(which == index, jnp.broadcast_to(part, (SUBLANES, LANES)), tile)

    def write(out, at, start):
        for source in (cross, mixed):
            for lane in range(0, half, LANES):
                out[at : at + rows, :] = source[pl.ds(start, rows), lane : lane + LANES]
                at += rows
        out[at : at + SUBLANES, :] = tile

    for out, start in zip(chunks, block_starts(rows, PARTNERS)):
        write(out, 0, start)


def update_kernel(gain, *refs):
    *arrays, gradient_ref, update_ref, mixed, cross = refs
    half = mixed.shape[0]
    rows = half // GROUP
    starts = iter(block_starts(rows, BLOCKS))
    length = arrays[0].shape[0]
    for source in arrays:
        for base in range(0, source.shape[0], length):
            start, at = next(starts), base
            for target in (cross, mixed):
                for lane in range(0, half, LANES):
                    target[pl.ds(start, rows), lane : lane + LANES] = source[at : at + rows, :]
                    at += rows
    diagonal = jnp.concatenate([source[at + i : at + i + 1, :] for i in range(half // LANES)], axis=1)
    row, column = grid_pair(half)
    on_diagonal = row == column
    packed = mixed[...]
    flipped = packed.T
    first = jnp.where(row <= column, packed, flipped)
    second = jnp.where(row > column, packed, flipped)
    second = jnp.where(on_diagonal, jnp.broadcast_to(diagonal, (half, half)), second)
    norm = jnp.sum(jnp.where(on_diagonal, first + second, 0.0), keepdims=True)
    divisor = jnp.sqrt(norm) + norm_floor
    scale = 1.0 / (divisor * divisor)
    gram = (first * scale, cross[...] * scale, second * scale)
    identity = jnp.where(on_diagonal, linear_term, 0.0)
    total = None
    for turn in range(ITERS):
        factor = Factor(gram)
        squared = factor.times(factor)
        polynomial = [cubic_term * g + quintic_term * q for g, q in zip(gram, squared)]
        polynomial = Factor((identity + polynomial[0], polynomial[1], identity + polynomial[2]))
        total = polynomial if total is None else Factor(total.times(polynomial))
        if turn + 1 < ITERS:
            gram = Factor(factor.times(polynomial)).times(polynomial)
    left = wide(gradient_ref[0], 1)
    for index in range(2):
        polished = dot(left, total.right[index])
        columns = slice(index * half, (index + 1) * half)
        update_ref[0, :, columns] = ((gain / divisor) * polished).astype(jnp.bfloat16)


def place_kernel(flipped, value_ref, *refs):
    whole_hbm, sem = refs[-2:]
    index = lax.axis_index("dp")
    copy = pltpu.make_async_copy(value_ref.at[0], whole_hbm.at[1 - index if flipped else index], sem)
    copy.start()
    copy.wait()


def on_device(mesh, gradient):
    pairs, size = mesh.shape["dp"], mesh.shape["tensor"]
    assert pairs % 2 == 0 and size % GROUP == 0 and size & (size - 1) == 0
    _, features, outputs = gradient.shape
    half = outputs // 2
    assert half // LANES <= SUBLANES
    length = 2 * half // GROUP * (half // LANES) + SUBLANES
    chunk = jax.ShapeDtypeStruct((length, LANES), jnp.float32)
    vmem = pl.BlockSpec(memory_space=pltpu.VMEM)
    anywhere = pl.BlockSpec(memory_space=pl.ANY)

    def swap(value, partner):
        return lax.ppermute(value, "tensor", [(i, i ^ partner) for i in range(size)])

    chunks = pl.pallas_call(
        gram_kernel,
        out_shape=[chunk] * GROUP,
        in_specs=[vmem],
        out_specs=[vmem] * GROUP,
        scratch_shapes=[pltpu.VMEM((half, half), jnp.float32)] * 2,
        compiler_params=pltpu.CompilerParams(vmem_limit_bytes=GRAM_VMEM),
        name="gram",
    )(gradient)
    owned = functools.reduce(jnp.add, [swap(value, k) for value, k in zip(chunks[1:], PARTNERS[1:])], chunks[0])
    step = GROUP
    while step < size:
        owned = owned + swap(owned, step)
        step *= 2
    relayed = swap(owned, RELAY)
    lone = [swap(owned, partner) for partner in LONE]
    pair = jnp.concatenate([owned, relayed])
    twice = [swap(pair, partner) for partner in TWICE]
    gathered = [owned, *twice, *lone, relayed]
    gain = update_gain * math.sqrt(max(FEATURES, OUTPUTS))
    update = pl.pallas_call(
        functools.partial(update_kernel, gain),
        out_shape=jax.ShapeDtypeStruct(gradient.shape, jnp.bfloat16),
        in_specs=[vmem] * (len(gathered) + 1),
        out_specs=vmem,
        scratch_shapes=[pltpu.VMEM((half, half), jnp.float32)] * 2,
        compiler_params=pltpu.CompilerParams(vmem_limit_bytes=UPDATE_VMEM),
        name="update",
    )(*gathered, gradient)
    if pairs != 2:
        return lax.all_gather(update, "dp", axis=0, tiled=True)

    def place(flipped, *operands):
        return pl.pallas_call(
            functools.partial(place_kernel, flipped),
            out_shape=jax.ShapeDtypeStruct((pairs, features, outputs), jnp.bfloat16),
            in_specs=[vmem, anywhere][: len(operands)],
            out_specs=anywhere,
            scratch_shapes=[pltpu.SemaphoreType.DMA],
            input_output_aliases={1: 0} if flipped else {},
            compiler_params=pltpu.CompilerParams(vmem_limit_bytes=PLACE_VMEM),
            cost_estimate=pl.CostEstimate(flops=PLACE_COST, bytes_accessed=2 * features * outputs, transcendentals=0),
            name="place",
        )(*operands)

    other = lax.ppermute(update, "dp", [(0, 1), (1, 0)])
    return place(True, other, place(False, update))


def solution(mesh):
    def body(gradient):
        return on_device(mesh, gradient)

    placed = (P("dp", "tensor", None),)
    return jax.shard_map(body, mesh=mesh, in_specs=placed, out_specs=P(None, "tensor", None), check_vma=False)
```

```python
import functools
import math

import jax
import jax.numpy as jnp
from jax import lax
from jax.experimental import pallas as pl
from jax.experimental.pallas import tpu as pltpu
from jax.sharding import PartitionSpec as P

FEATURES = 8192
OUTPUTS = 512
ITERS = 3

linear_term = 3.4445
cubic_term = -4.775
quintic_term = 2.0315
norm_floor = 1e-07
update_gain = 0.2

LANES = 128
GRAM_VMEM = 16 << 20
UPDATE_VMEM = 32 << 20
PLACE_COST = 1 << 20
PLACE_VMEM = 4 << 20
SUBLANES = 8


GROUP = 8
RELAY = 4
LONE = (3, 7)
TWICE = (2, 1)
BLOCKS = (0, *[block for partner in TWICE for block in (partner, partner ^ RELAY)], *LONE, RELAY)
OUT_TWICE = (2,)
OUT_LONE = (7, 5, 3, 1)
OUT_BLOCKS = (0, *[block for partner in OUT_TWICE for block in (partner, partner ^ RELAY)], *OUT_LONE, RELAY)


def split(value):
    high = value.astype(jnp.bfloat16)
    low = (value - high.astype(jnp.float32)).astype(jnp.bfloat16)
    return high, low


def wide(value, axis):
    high, low = split(value)
    return jnp.concatenate([high, high, low] if axis == 1 else [high, low, high], axis=axis)


def dot(first, second, contract=(1, 0)):
    return lax.dot_general(
        first, second, (((contract[0],), (contract[1],)), ((), ())), preferred_element_type=jnp.float32
    )


class Factor:
    def __init__(self, blocks):
        (high_a, low_a), (high_b, low_b), (high_c, low_c) = [split(block) for block in blocks]
        turned_high, turned_low = high_b.T, low_b.T
        rows = [((high_a, high_b), (low_a, low_b)), ((turned_high, high_c), (turned_low, low_c))]
        columns = [((high_a, turned_high), (low_a, turned_low)), ((high_b, high_c), (low_b, low_c))]
        self.left = [jnp.concatenate([*high, *high, *low], axis=1) for high, low in rows]
        self.right = [jnp.concatenate([*high, *low, *high], axis=0) for high, low in columns]

    def times(self, other):
        return [dot(self.left[i], other.right[j]) for i, j in ((0, 0), (0, 1), (1, 1))]


def grid_pair(half):
    shape = (half, half)
    return lax.broadcasted_iota(jnp.int32, shape, 0), lax.broadcasted_iota(jnp.int32, shape, 1)


def block_starts(rows, order):
    me = lax.rem(lax.axis_index("tensor"), GROUP)
    return [pl.multiple_of((me ^ partner) * rows, rows) for partner in order]


def gram_kernel(gradient_ref, *refs):
    *arrays, mixed, cross = refs
    half = mixed.shape[0]
    rows = half // GROUP
    high, low = split(gradient_ref[0])
    left = jnp.concatenate([high, high, low], axis=0)
    right = jnp.concatenate([high, low, high], axis=0)
    first = dot(left[:, :half], right[:, :half], (0, 0))
    cross[...] = dot(left[:, :half], right[:, half:], (0, 0))
    second = dot(left[:, half:], right[:, half:], (0, 0))
    row, column = grid_pair(half)
    mixed[...] = jnp.where(row <= column, first, second)
    diagonal = jnp.sum(jnp.where(row == column, second, 0.0), axis=0, keepdims=True)
    which = lax.broadcasted_iota(jnp.int32, (SUBLANES, LANES), 0)
    tile = jnp.zeros((SUBLANES, LANES), jnp.float32)
    for index in range(half // LANES):
        part = diagonal[:, index * LANES : (index + 1) * LANES]
        tile = jnp.where(which == index, jnp.broadcast_to(part, (SUBLANES, LANES)), tile)

    def write(out, at, start):
        for source in (cross, mixed):
            for lane in range(0, half, LANES):
                out[at : at + rows, :] = source[pl.ds(start, rows), lane : lane + LANES]
                at += rows
        out[at : at + SUBLANES, :] = tile

    starts = iter(block_starts(rows, OUT_BLOCKS))
    length = arrays[0].shape[0]
    for out in arrays:
        for base in range(0, out.shape[0], length):
            write(out, base, next(starts))


def update_kernel(gain, *refs):
    *arrays, gradient_ref, update_ref, mixed, cross = refs
    half = mixed.shape[0]
    rows = half // GROUP
    starts = iter(block_starts(rows, BLOCKS))
    length = arrays[0].shape[0]
    for source in arrays:
        for base in range(0, source.shape[0], length):
            start, at = next(starts), base
            for target in (cross, mixed):
                for lane in range(0, half, LANES):
                    target[pl.ds(start, rows), lane : lane + LANES] = source[at : at + rows, :]
                    at += rows
    diagonal = jnp.concatenate([source[at + i : at + i + 1, :] for i in range(half // LANES)], axis=1)
    row, column = grid_pair(half)
    on_diagonal = row == column
    packed = mixed[...]
    flipped = packed.T
    first = jnp.where(row <= column, packed, flipped)
    second = jnp.where(row > column, packed, flipped)
    second = jnp.where(on_diagonal, jnp.broadcast_to(diagonal, (half, half)), second)
    norm = jnp.sum(jnp.where(on_diagonal, first + second, 0.0), keepdims=True)
    divisor = jnp.sqrt(norm) + norm_floor
    scale = 1.0 / (divisor * divisor)
    gram = (first * scale, cross[...] * scale, second * scale)
    identity = jnp.where(on_diagonal, linear_term, 0.0)
    total = None
    for turn in range(ITERS):
        factor = Factor(gram)
        squared = factor.times(factor)
        polynomial = [cubic_term * g + quintic_term * q for g, q in zip(gram, squared)]
        polynomial = Factor((identity + polynomial[0], polynomial[1], identity + polynomial[2]))
        total = polynomial if total is None else Factor(total.times(polynomial))
        if turn + 1 < ITERS:
            gram = Factor(factor.times(polynomial)).times(polynomial)
    left = wide(gradient_ref[0], 1)
    for index in range(2):
        polished = dot(left, total.right[index])
        columns = slice(index * half, (index + 1) * half)
        update_ref[0, :, columns] = ((gain / divisor) * polished).astype(jnp.bfloat16)


def place_kernel(flipped, value_ref, *refs):
    whole_hbm, sem = refs[-2:]
    index = lax.axis_index("dp")
    copy = pltpu.make_async_copy(value_ref.at[0], whole_hbm.at[1 - index if flipped else index], sem)
    copy.start()
    copy.wait()


def on_device(mesh, gradient):
    pairs, size = mesh.shape["dp"], mesh.shape["tensor"]
    assert pairs % 2 == 0 and size % GROUP == 0 and size & (size - 1) == 0
    _, features, outputs = gradient.shape
    half = outputs // 2
    assert half // LANES <= SUBLANES
    length = 2 * half // GROUP * (half // LANES) + SUBLANES
    chunk = jax.ShapeDtypeStruct((length, LANES), jnp.float32)
    vmem = pl.BlockSpec(memory_space=pltpu.VMEM)
    anywhere = pl.BlockSpec(memory_space=pl.ANY)

    def swap(value, partner):
        return lax.ppermute(value, "tensor", [(i, i ^ partner) for i in range(size)])

    double = jax.ShapeDtypeStruct((2 * length, LANES), jnp.float32)
    shapes = [chunk] + [double] * len(OUT_TWICE) + [chunk] * (len(OUT_LONE) + 1)
    keep, *chunks, relayed = pl.pallas_call(
        gram_kernel,
        out_shape=shapes,
        in_specs=[vmem],
        out_specs=[vmem] * len(shapes),
        scratch_shapes=[pltpu.VMEM((half, half), jnp.float32)] * 2,
        compiler_params=pltpu.CompilerParams(vmem_limit_bytes=GRAM_VMEM),
        name="gram",
    )(gradient)
    arrived = [swap(value, partner) for value, partner in zip(chunks, OUT_TWICE + OUT_LONE)]
    twice, lone = arrived[: len(OUT_TWICE)], arrived[len(OUT_TWICE) :]
    relayed = functools.reduce(jnp.add, [value[length:] for value in twice], relayed)
    owned = functools.reduce(jnp.add, [value[:length] for value in twice] + lone, keep)
    owned = owned + swap(relayed, RELAY)
    step = GROUP
    while step < size:
        owned = owned + swap(owned, step)
        step *= 2
    relayed = swap(owned, RELAY)
    lone = [swap(owned, partner) for partner in LONE]
    pair = jnp.concatenate([owned, relayed])
    twice = [swap(pair, partner) for partner in TWICE]
    gathered = [owned, *twice, *lone, relayed]
    gain = update_gain * math.sqrt(max(FEATURES, OUTPUTS))
    update = pl.pallas_call(
        functools.partial(update_kernel, gain),
        out_shape=jax.ShapeDtypeStruct(gradient.shape, jnp.bfloat16),
        in_specs=[vmem] * (len(gathered) + 1),
        out_specs=vmem,
        scratch_shapes=[pltpu.VMEM((half, half), jnp.float32)] * 2,
        compiler_params=pltpu.CompilerParams(vmem_limit_bytes=UPDATE_VMEM),
        name="update",
    )(*gathered, gradient)
    if pairs != 2:
        return lax.all_gather(update, "dp", axis=0, tiled=True)

    def place(flipped, *operands):
        return pl.pallas_call(
            functools.partial(place_kernel, flipped),
            out_shape=jax.ShapeDtypeStruct((pairs, features, outputs), jnp.bfloat16),
            in_specs=[vmem, anywhere][: len(operands)],
            out_specs=anywhere,
            scratch_shapes=[pltpu.SemaphoreType.DMA],
            input_output_aliases={1: 0} if flipped else {},
            compiler_params=pltpu.CompilerParams(vmem_limit_bytes=PLACE_VMEM),
            cost_estimate=pl.CostEstimate(flops=PLACE_COST, bytes_accessed=2 * features * outputs, transcendentals=0),
            name="place",
        )(*operands)

    other = lax.ppermute(update, "dp", [(0, 1), (1, 0)])
    return place(True, other, place(False, update))


def solution(mesh):
    def body(gradient):
        return on_device(mesh, gradient)

    placed = (P("dp", "tensor", None),)
    return jax.shard_map(body, mesh=mesh, in_specs=placed, out_specs=P(None, "tensor", None), check_vma=False)
```

```python
import functools
import math

import jax
import jax.numpy as jnp
from jax import lax
from jax.experimental import pallas as pl
from jax.experimental.pallas import tpu as pltpu
from jax.sharding import PartitionSpec as P

FEATURES = 8192
OUTPUTS = 512
ITERS = 3

linear_term = 3.4445
cubic_term = -4.775
quintic_term = 2.0315
norm_floor = 1e-07
update_gain = 0.2

LANES = 128
GRAM_VMEM = 16 << 20
UPDATE_VMEM = 32 << 20
PLACE_COST = 1 << 20
PLACE_VMEM = 4 << 20
SUBLANES = 8


GROUP = 8
RELAY = 4
LONE = (3, 7)
TWICE = (2, 1)
BLOCKS = (0, *[block for partner in TWICE for block in (partner, partner ^ RELAY)], *LONE, RELAY)
OUT_RELAY = 2
OUT_TWICE = (1,)
OUT_LONE = (7, 6, 5, 4)
OUT_BLOCKS = (0, *[block for partner in OUT_TWICE for block in (partner, partner ^ OUT_RELAY)], *OUT_LONE, OUT_RELAY)


def split(value):
    high = value.astype(jnp.bfloat16)
    low = (value - high.astype(jnp.float32)).astype(jnp.bfloat16)
    return high, low


def wide(value, axis):
    high, low = split(value)
    return jnp.concatenate([high, high, low] if axis == 1 else [high, low, high], axis=axis)


def dot(first, second, contract=(1, 0)):
    return lax.dot_general(
        first, second, (((contract[0],), (contract[1],)), ((), ())), preferred_element_type=jnp.float32
    )


class Factor:
    def __init__(self, blocks):
        (high_a, low_a), (high_b, low_b), (high_c, low_c) = [split(block) for block in blocks]
        turned_high, turned_low = high_b.T, low_b.T
        rows = [((high_a, high_b), (low_a, low_b)), ((turned_high, high_c), (turned_low, low_c))]
        columns = [((high_a, turned_high), (low_a, turned_low)), ((high_b, high_c), (low_b, low_c))]
        self.left = [jnp.concatenate([*high, *high, *low], axis=1) for high, low in rows]
        self.right = [jnp.concatenate([*high, *low, *high], axis=0) for high, low in columns]

    def times(self, other):
        return [dot(self.left[i], other.right[j]) for i, j in ((0, 0), (0, 1), (1, 1))]


def grid_pair(half):
    shape = (half, half)
    return lax.broadcasted_iota(jnp.int32, shape, 0), lax.broadcasted_iota(jnp.int32, shape, 1)


def block_starts(rows, order):
    me = lax.rem(lax.axis_index("tensor"), GROUP)
    return [pl.multiple_of((me ^ partner) * rows, rows) for partner in order]


def gram_kernel(gradient_ref, *refs):
    *arrays, mixed, cross = refs
    half = mixed.shape[0]
    rows = half // GROUP
    high, low = split(gradient_ref[0])
    left = jnp.concatenate([high, high, low], axis=0)
    right = jnp.concatenate([high, low, high], axis=0)
    first = dot(left[:, :half], right[:, :half], (0, 0))
    cross[...] = dot(left[:, :half], right[:, half:], (0, 0))
    second = dot(left[:, half:], right[:, half:], (0, 0))
    row, column = grid_pair(half)
    mixed[...] = jnp.where(row <= column, first, second)
    diagonal = jnp.sum(jnp.where(row == column, second, 0.0), axis=0, keepdims=True)
    which = lax.broadcasted_iota(jnp.int32, (SUBLANES, LANES), 0)
    tile = jnp.zeros((SUBLANES, LANES), jnp.float32)
    for index in range(half // LANES):
        part = diagonal[:, index * LANES : (index + 1) * LANES]
        tile = jnp.where(which == index, jnp.broadcast_to(part, (SUBLANES, LANES)), tile)

    def write(out, at, start):
        for source in (cross, mixed):
            for lane in range(0, half, LANES):
                out[at : at + rows, :] = source[pl.ds(start, rows), lane : lane + LANES]
                at += rows
        out[at : at + SUBLANES, :] = tile

    starts = iter(block_starts(rows, OUT_BLOCKS))
    length = arrays[0].shape[0]
    for out in arrays:
        for base in range(0, out.shape[0], length):
            write(out, base, next(starts))


def update_kernel(gain, *refs):
    *arrays, gradient_ref, update_ref, mixed, cross = refs
    half = mixed.shape[0]
    rows = half // GROUP
    starts = iter(block_starts(rows, BLOCKS))
    length = arrays[0].shape[0]
    for source in arrays:
        for base in range(0, source.shape[0], length):
            start, at = next(starts), base
            for target in (cross, mixed):
                for lane in range(0, half, LANES):
                    target[pl.ds(start, rows), lane : lane + LANES] = source[at : at + rows, :]
                    at += rows
    diagonal = jnp.concatenate([source[at + i : at + i + 1, :] for i in range(half // LANES)], axis=1)
    row, column = grid_pair(half)
    on_diagonal = row == column
    packed = mixed[...]
    flipped = packed.T
    first = jnp.where(row <= column, packed, flipped)
    second = jnp.where(row > column, packed, flipped)
    second = jnp.where(on_diagonal, jnp.broadcast_to(diagonal, (half, half)), second)
    norm = jnp.sum(jnp.where(on_diagonal, first + second, 0.0), keepdims=True)
    divisor = jnp.sqrt(norm) + norm_floor
    scale = 1.0 / (divisor * divisor)
    gram = (first * scale, cross[...] * scale, second * scale)
    identity = jnp.where(on_diagonal, linear_term, 0.0)
    total = None
    for turn in range(ITERS):
        factor = Factor(gram)
        squared = factor.times(factor)
        polynomial = [cubic_term * g + quintic_term * q for g, q in zip(gram, squared)]
        polynomial = Factor((identity + polynomial[0], polynomial[1], identity + polynomial[2]))
        total = polynomial if total is None else Factor(total.times(polynomial))
        if turn + 1 < ITERS:
            gram = Factor(factor.times(polynomial)).times(polynomial)
    left = wide(gradient_ref[0], 1)
    for index in range(2):
        polished = dot(left, total.right[index])
        columns = slice(index * half, (index + 1) * half)
        update_ref[0, :, columns] = ((gain / divisor) * polished).astype(jnp.bfloat16)


def place_kernel(flipped, value_ref, *refs):
    whole_hbm, sem = refs[-2:]
    index = lax.axis_index("dp")
    copy = pltpu.make_async_copy(value_ref.at[0], whole_hbm.at[1 - index if flipped else index], sem)
    copy.start()
    copy.wait()


def on_device(mesh, gradient):
    pairs, size = mesh.shape["dp"], mesh.shape["tensor"]
    assert pairs % 2 == 0 and size % GROUP == 0 and size & (size - 1) == 0
    _, features, outputs = gradient.shape
    half = outputs // 2
    assert half // LANES <= SUBLANES
    length = 2 * half // GROUP * (half // LANES) + SUBLANES
    chunk = jax.ShapeDtypeStruct((length, LANES), jnp.float32)
    vmem = pl.BlockSpec(memory_space=pltpu.VMEM)
    anywhere = pl.BlockSpec(memory_space=pl.ANY)

    def swap(value, partner):
        return lax.ppermute(value, "tensor", [(i, i ^ partner) for i in range(size)])

    double = jax.ShapeDtypeStruct((2 * length, LANES), jnp.float32)
    shapes = [chunk] + [double] * len(OUT_TWICE) + [chunk] * (len(OUT_LONE) + 1)
    keep, *chunks, relayed = pl.pallas_call(
        gram_kernel,
        out_shape=shapes,
        in_specs=[vmem],
        out_specs=[vmem] * len(shapes),
        scratch_shapes=[pltpu.VMEM((half, half), jnp.float32)] * 2,
        compiler_params=pltpu.CompilerParams(vmem_limit_bytes=GRAM_VMEM),
        name="gram",
    )(gradient)
    arrived = [swap(value, partner) for value, partner in zip(chunks, OUT_TWICE + OUT_LONE)]
    twice, lone = arrived[: len(OUT_TWICE)], arrived[len(OUT_TWICE) :]
    relayed = functools.reduce(jnp.add, [value[length:] for value in twice], relayed)
    owned = functools.reduce(jnp.add, [value[:length] for value in twice] + lone, keep)
    owned = owned + swap(relayed, OUT_RELAY)
    step = GROUP
    while step < size:
        owned = owned + swap(owned, step)
        step *= 2
    relayed = swap(owned, RELAY)
    lone = [swap(owned, partner) for partner in LONE]
    pair = jnp.concatenate([owned, relayed])
    twice = [swap(pair, partner) for partner in TWICE]
    gathered = [owned, *twice, *lone, relayed]
    gain = update_gain * math.sqrt(max(FEATURES, OUTPUTS))
    update = pl.pallas_call(
        functools.partial(update_kernel, gain),
        out_shape=jax.ShapeDtypeStruct(gradient.shape, jnp.bfloat16),
        in_specs=[vmem] * (len(gathered) + 1),
        out_specs=vmem,
        scratch_shapes=[pltpu.VMEM((half, half), jnp.float32)] * 2,
        compiler_params=pltpu.CompilerParams(vmem_limit_bytes=UPDATE_VMEM),
        name="update",
    )(*gathered, gradient)
    if pairs != 2:
        return lax.all_gather(update, "dp", axis=0, tiled=True)

    def place(flipped, *operands):
        return pl.pallas_call(
            functools.partial(place_kernel, flipped),
            out_shape=jax.ShapeDtypeStruct((pairs, features, outputs), jnp.bfloat16),
            in_specs=[vmem, anywhere][: len(operands)],
            out_specs=anywhere,
            scratch_shapes=[pltpu.SemaphoreType.DMA],
            input_output_aliases={1: 0} if flipped else {},
            compiler_params=pltpu.CompilerParams(vmem_limit_bytes=PLACE_VMEM),
            cost_estimate=pl.CostEstimate(flops=PLACE_COST, bytes_accessed=2 * features * outputs, transcendentals=0),
            name="place",
        )(*operands)

    other = lax.ppermute(update, "dp", [(0, 1), (1, 0)])
    return place(True, other, place(False, update))


def solution(mesh):
    def body(gradient):
        return on_device(mesh, gradient)

    placed = (P("dp", "tensor", None),)
    return jax.shard_map(body, mesh=mesh, in_specs=placed, out_specs=P(None, "tensor", None), check_vma=False)
```
